128 devices in a mesh: seq: 8 (over z, core), grp: 16 (over y, x).
Axes of the slice: x: 4, y: 4, z: 4, core: 2. Of those that a mesh axis runs over, the one named last changes fastest.
Arguments:
- hidden_in: bfloat16 [16, 4096, 1024], P('grp', 'seq'), may hold values from -64 to 64, as said below
- lengths: int32 [16], P('grp'), may hold values from 512 to 4096
- project_weight: bfloat16 [1024, 3072], replicated, may hold values from -0.1875 to 0.1875
- output_weight: bfloat16 [1024, 1024], replicated, may hold values from -0.1875 to 0.1875
- first_gain: float32 [1024], replicated, may hold values from 0.5 to 1.5
- first_shift: float32 [1024], replicated, may hold values from -3 to 3
- up_weight: bfloat16 [1024, 4096], P('grp'), may hold values from -0.1875 to 0.1875
- down_weight: bfloat16 [1024, 4096], P('grp'), may hold values from -0.09375 to 0.09375
- second_gain: float32 [1024], replicated, may hold values from 0.5 to 1.5
- second_shift: float32 [1024], replicated, may hold values from -3 to 3
- queries: float32 [128, 1024], P('grp'), may hold values from -6 to 6
- positive: int32 [128], P('grp'), may hold values from 0 to 15
Outputs:
- hidden_out: bfloat16 [16, 4096, 1024], P('grp', 'seq')
- embeddings: float32 [16, 1024], P('grp')
- query_loss: float32 [128], P('grp')
The draws below stay inside these ranges and needn't reach their ends.
Inputs may be any that keep to these rules, and one draw needn't show every extreme that they name: `hidden_in`: activations.
All inputs are finite; a program needn't handle non-finite values.
Results may differ from the reference program's by a relative error of at most 0.0076.
Values may be sent and summed in bfloat16 or wider, within the bound.
A program may use at most 192 MiB of HBM per device.

```python
import math
import jax
import jax.numpy as jnp
from jax import lax

D = 1024
HEADS = 16
HEAD_DIM = 64
FF = 4096
LEN = 4096
PASSAGES = 16
QUERIES = 128


def draw_hidden_in(key, part):
    base = jnp.clip(jax.random.normal(key, (PASSAGES, LEN, D), jnp.float32), -6.0, 6.0)
    return base.astype(jnp.bfloat16)


def plant(drawn, own_key, least, high):
    spot = [jax.random.randint(jax.random.fold_in(own_key, axis), (), 0, length) for axis, length in enumerate(drawn.shape)]
    main_axis = drawn.shape.index(max(drawn.shape))
    neighbour = spot[:main_axis] + [(spot[main_axis] + 1) % drawn.shape[main_axis]] + spot[main_axis + 1:]
    return drawn.at[tuple(spot)].set(least).at[tuple(neighbour)].set(high)


def shard_levels(stream_key, dims, shards, low, top_value):
    def one(position, parts):
        draws = jax.random.uniform(jax.random.fold_in(jax.random.fold_in(stream_key, 6), position), (parts,), jnp.float32, low / len(shards), top_value / len(shards))
        return jnp.repeat(jnp.exp(draws), dims[position] // parts).reshape((-1,) + (1,) * (len(dims) - position - 1))

    factor_of = one(*shards[0])
    for cut in shards[1:]:
        factor_of = factor_of * one(*cut)
    return factor_of


def bell_draw(stream_key, dims, width, most, shards=(), kind=jnp.bfloat16):
    level = shard_levels(stream_key, dims, shards, -0.22, 0.18) if shards else 1.0
    values = jax.random.normal(stream_key, dims, jnp.float32) * width * level
    return jnp.minimum(jnp.maximum(values, -most), most).astype(kind)


def setup_inputs(seed: int = 0) -> dict:
    arg_keys = jax.random.split(jax.random.key(seed), 13)
    hidden_in = draw_hidden_in(jax.random.fold_in(arg_keys[12], 71), 0)
    lengths = plant(jax.random.randint(arg_keys[1], (PASSAGES,), LEN // 8, LEN + 1), jax.random.fold_in(arg_keys[1], 1), LEN // 8, LEN).astype(jnp.int32)
    project_weight = bell_draw(arg_keys[2], (D, 3 * D), D ** -0.5, 0.1875)
    output_weight = bell_draw(arg_keys[3], (D, D), D ** -0.5, 0.1875)
    first_gain = jnp.clip(1.0 + 0.1 * jax.random.normal(arg_keys[4], (D,), jnp.float32), 0.5, 1.5)
    first_shift = bell_draw(arg_keys[5], (D,), 0.5, 3.0, (), jnp.float32)
    up_weight = bell_draw(arg_keys[6], (D, FF), D ** -0.5, 0.1875, ((0, 16),))
    down_weight = bell_draw(arg_keys[7], (D, FF), FF ** -0.5, 0.09375, ((0, 16),))
    second_gain = jnp.clip(1.0 + 0.1 * jax.random.normal(arg_keys[8], (D,), jnp.float32), 0.5, 1.5)
    second_shift = bell_draw(arg_keys[9], (D,), 0.5, 3.0, (), jnp.float32)
    queries = bell_draw(arg_keys[10], (QUERIES, D), 1.0, 6.0, ((0, 16),), jnp.float32)
    positive = plant(jax.random.randint(arg_keys[11], (QUERIES,), 0, PASSAGES), jax.random.fold_in(arg_keys[11], 1), 0, PASSAGES - 1).astype(jnp.int32)
    return {"hidden_in": hidden_in, "lengths": lengths, "project_weight": project_weight, "output_weight": output_weight, "first_gain": first_gain, "first_shift": first_shift, "up_weight": up_weight, "down_weight": down_weight, "second_gain": second_gain, "second_shift": second_shift, "queries": queries, "positive": positive}


def layer_norm(values, gain, shift):
    average = lax.optimization_barrier(jnp.mean(values, axis=-1, keepdims=True))
    centred = values - average
    variance = lax.optimization_barrier(jnp.mean(centred * centred, axis=-1, keepdims=True))
    return centred * lax.rsqrt(variance + 1e-05) * gain + shift

def attend(projected, length):
    block = min(1024, LEN)
    query_all = projected[:, :D].reshape(LEN, HEADS, HEAD_DIM).astype(jnp.float32)
    key_all = projected[:, D:2 * D].reshape(LEN, HEADS, HEAD_DIM).astype(jnp.float32)
    value_all = projected[:, 2 * D:].reshape(LEN, HEADS, HEAD_DIM).astype(jnp.float32)
    key_valid = jnp.arange(LEN, dtype=jnp.int32) < length
    scale = 1.0 / math.sqrt(HEAD_DIM)

    def one_block(index):
        query_rows = lax.dynamic_slice_in_dim(query_all, (index * block).astype(jnp.int32), block, 0)
        scores = jnp.einsum('qhd,khd->hqk', query_rows, key_all) * scale
        scores = jnp.where(key_valid[None, None, :], scores, -jnp.inf)
        highest = lax.optimization_barrier(jnp.max(scores, axis=-1, keepdims=True))
        expo = jnp.exp(scores - highest)
        probs = (expo / lax.optimization_barrier(jnp.sum(expo, axis=-1, keepdims=True))).astype(jnp.bfloat16)
        result = jnp.einsum('hqk,khd->qhd', probs.astype(jnp.float32), value_all)
        return result.astype(jnp.bfloat16).reshape(block, D)
    blocks = lax.map(one_block, jnp.arange(LEN // block, dtype=jnp.int32))
    return blocks.reshape(LEN, D)

def reference(hidden_in, lengths, project_weight, output_weight, first_gain, first_shift, up_weight, down_weight, second_gain, second_shift, queries, positive):

    def encode(item):
        tokens, length = item
        projected = jnp.dot(tokens, project_weight, preferred_element_type=jnp.float32).astype(jnp.bfloat16)
        attended = attend(projected, length)
        mixed = jnp.dot(attended, output_weight, preferred_element_type=jnp.float32) + tokens.astype(jnp.float32)
        normed = layer_norm(mixed, first_gain, first_shift).astype(jnp.bfloat16)
        inner = jax.nn.gelu(jnp.dot(normed, up_weight, preferred_element_type=jnp.float32), approximate=False).astype(jnp.bfloat16)
        outer = lax.dot_general(inner, down_weight, (((1,), (1,)), ((), ())), preferred_element_type=jnp.float32)
        final = layer_norm(outer + normed.astype(jnp.float32), second_gain, second_shift)
        valid = (jnp.arange(LEN, dtype=jnp.int32) < length).astype(jnp.float32)
        pooled = lax.optimization_barrier(jnp.sum(final * valid[:, None], axis=0)) / length.astype(jnp.float32)
        return (final.astype(jnp.bfloat16), pooled)
    hidden_out, pooled = lax.map(encode, (hidden_in, lengths))
    embeddings = pooled / jnp.sqrt(lax.optimization_barrier(jnp.sum(pooled * pooled, axis=-1, keepdims=True)) + 1e-06)
    short_queries = (queries / jnp.sqrt(lax.optimization_barrier(jnp.sum(queries * queries, axis=-1, keepdims=True)) + 1e-06)).astype(jnp.bfloat16)
    short_passages = embeddings.astype(jnp.bfloat16)
    logits = 20.0 * jnp.dot(short_queries, short_passages.T, preferred_element_type=jnp.float32)
    chosen = positive[:, None] == jnp.arange(PASSAGES, dtype=jnp.int32)[None, :]
    picked = lax.optimization_barrier(jnp.sum(jnp.where(chosen, logits, 0.0), axis=1))
    query_loss = jnp.log(lax.optimization_barrier(jnp.sum(jnp.exp(logits), axis=1))) - picked
    return (hidden_out, embeddings, query_loss)
```

```python
import math
import functools

import jax
import jax.numpy as jnp
from jax import lax
from jax.experimental import pallas as pl
from jax.experimental.pallas import tpu as pltpu
from jax.sharding import PartitionSpec as P

MESH = pl.DeviceIdType.MESH
BF = jnp.bfloat16
F32 = jnp.float32
NEG = -1e30
KB = 1024
QT = 512
NT = 1024 // QT
TILES = 8 * NT
U = 4
ITERS = TILES // U
SCALE = math.log2(math.e) / 8.0


def attend_kernel(
    len_ref, x_ref, w_ref, up_ref, dn_ref, att_ref, wf_ref,
    xbuf, wqkv, kscr, vscr, qscr, acc, mx, s_a, s_b, al, stage, wv,
    lsem, hs, hr, ds, dr, ws, wr, ps, pr, osem,
):
    s = lax.axis_index("seq")
    g = lax.axis_index("grp")
    c = lax.rem(s, 2)
    z = s // 2
    gx = lax.rem(g, 4)
    gy = g // 4
    mate = {"seq": s + 1 - 2 * c}
    zup = {"seq": lax.rem(s + 2, 8)}
    zdn = {"seq": lax.rem(s + 6, 8)}

    def wrap(v):
        return lax.rem(v, 4)

    def peer(axis, step):
        if axis == 0:
            return {"grp": gy * 4 + wrap(gx + step)}
        return {"grp": wrap(gy + step) * 4 + gx}

    loads = [pltpu.make_async_copy(x_ref, xbuf.at[0, pl.ds(0, 512)], lsem.at[0])]
    for t in range(3):
        cols = pl.ds(pl.multiple_of(t * 1024 + c * 512, 512), 512)
        loads.append(
            pltpu.make_async_copy(w_ref.at[:, cols], wqkv.at[:, pl.ds(t * 512, 512)], lsem.at[1 + t])
        )
    loads.append(pltpu.make_async_copy(up_ref, wv.at[0], lsem.at[4]))
    loads.append(pltpu.make_async_copy(dn_ref, wv.at[1], lsem.at[5]))
    for cp in loads:
        cp.start()

    peers = [mate, zup, zdn, peer(0, 1), peer(0, 3), peer(1, 1), peer(1, 3)]
    barrier = pltpu.get_barrier_semaphore()
    for d in peers:
        pl.semaphore_signal(barrier, inc=1, device_id=d, device_id_type=MESH)
    pl.semaphore_wait(barrier, len(peers))

    def rcopy(src, dst, ssem, rsem, dev):
        return pltpu.make_async_remote_copy(
            src_ref=src, dst_ref=dst, send_sem=ssem, recv_sem=rsem, device_id=dev, device_id_type=MESH
        )

    def h_piece(p):
        return xbuf.at[0, pl.ds(p * 256, 256)]

    def x_quarter(j, q):
        return xbuf.at[j, pl.ds(q * 256, 256)]

    h_own = rcopy(xbuf.at[0, pl.ds(0, 512)], xbuf.at[0, pl.ds(512, 512)], ds.at[0], dr.at[0], mate)
    h_dn = [rcopy(h_piece(p), x_quarter(1 + p, 0), hs.at[p], hr.at[p], zdn) for p in range(2)]
    h_up = [rcopy(h_piece(p), x_quarter(1 + p, 2), hs.at[2 + p], hr.at[2 + p], zup) for p in range(2)]
    f_dn = rcopy(x_quarter(1, 0), x_quarter(3, 0), hs.at[4], hr.at[4], zdn)
    f_up = rcopy(x_quarter(2, 2), x_quarter(3, 1), hs.at[5], hr.at[5], zup)
    h_mate = []
    for k, (j, a, b) in enumerate([(1, 0, 1), (1, 2, 3), (2, 0, 1), (2, 2, 3), (3, 0, 2), (3, 1, 3)]):
        h_mate.append(rcopy(x_quarter(j, a), x_quarter(j, b), ds.at[1 + k], dr.at[1 + k], mate))

    def origin_row(t, d1, d2):
        dx, dy = (d1, d2) if t == 0 else (d2, d1)
        return (wrap(gy + dy) * 4 + wrap(gx + dx)) * 64 + t * 32

    def w_reg(t, d1, d2, lo, n):
        return wf_ref.at[c, pl.ds(pl.multiple_of(origin_row(t, d1, d2) + lo, 16), n), :]

    w1, w2, w3, w4 = {}, {}, {}, {}
    for t in range(2):
        mine = wv.at[c, pl.ds(t * 32, 32), :]
        a1, a2 = t, 1 - t
        for i, (step, seen) in enumerate([(1, 3), (3, 1)]):
            w1[t, i] = rcopy(mine, w_reg(t, 0, 0, 0, 32), ws.at[t, i], wr.at[t, seen, 0, 0], peer(a1, step))
            w2[t, i] = rcopy(
                w_reg(t, seen, 0, 16 * i, 16), w_reg(t, seen, 0, 16 * i, 16),
                ws.at[t, 2 + i], wr.at[t, 2, 0, i], peer(a1, step),
            )
            for d1 in range(4):
                src = mine if d1 == 0 else w_reg(t, d1, 0, 0, 32)
                w3[t, d1, i] = rcopy(
                    src, w_reg(t, d1, 0, 0, 32), ws.at[t, 4 + 2 * d1 + i], wr.at[t, d1, seen, 0], peer(a2, step)
                )
                w4[t, d1, i] = rcopy(
                    w_reg(t, d1, seen, 16 * i, 16), w_reg(t, d1, seen, 16 * i, 16),
                    ws.at[t, 12 + 2 * d1 + i], wr.at[t, d1, 2, i], peer(a2, step),
                )
    w5 = {}
    for t in range(2):
        for d1 in range(4):
            for d2 in range(4):
                if d1 or d2:
                    w5[t, d1, d2] = rcopy(
                        w_reg(t, d1, d2, 0, 32), w_reg(t, d1, d2, 0, 32),
                        ps.at[t, d1, d2], pr.at[t, d1, d2], mate,
                    )

    def w_arrived(t, d1, d2, k, n):
        reg = w_reg(t, d1, d2, 16 * k, n)
        pltpu.make_async_copy(reg, reg, wr.at[t, d1, d2, k]).wait()

    loads[0].wait()
    for cp in h_dn + h_up + [h_own]:
        cp.start()
    loads[4].wait()
    loads[5].wait()
    for t in range(2):
        for i in range(2):
            w1[t, i].start()
    for t in range(2):
        for i in range(2):
            w3[t, 0, i].start()
    own_rows = pl.ds(pl.multiple_of(g * 64, 64), 64)
    outs = [pltpu.make_async_copy(wv.at[k], wf_ref.at[k, own_rows, :], lsem.at[6 + k]) for k in range(2)]
    for cp in outs:
        cp.start()

    qscr[...] = jnp.zeros_like(qscr)
    for h in range(8):
        qscr[h, 128:144, :] = (lax.broadcasted_iota(jnp.int32, (16, KB), 0) == 0).astype(BF)
        vscr[h, 64:80, :] = jnp.ones((16, KB), BF)
    acc[...] = jnp.zeros_like(acc)
    mx[...] = jnp.full_like(mx, NEG)
    length = len_ref[0]

    for k in range(3):
        loads[1 + k].wait()
    h_own.wait_recv()
    for i in range(2):
        q = jnp.dot(xbuf[0], wqkv[:, 256 * i : 256 * i + 256], preferred_element_type=F32)
        qt = (q * SCALE).T.astype(BF)
        for u in range(4):
            h = 4 * i + u
            qscr[h, (u % 2) * 64 : (u % 2) * 64 + 64, :] = qt[64 * u : 64 * u + 64]

    bufs = [s_a, s_b]

    def scores(h, t, sref, slot):
        sl = pl.ds(pl.multiple_of(t * QT, QT), QT)
        sc = jnp.dot(kscr[h // 2], qscr[h, :, sl], preferred_element_type=F32)
        sref[...] = sc
        old = mx[h, :, sl]
        new = jnp.maximum(old, jnp.max(sc, axis=0, keepdims=True))
        mx[h, :, sl] = new
        al[slot] = jnp.exp2(old - new)
        al[slot + 2] = new

    def values(h, t, sref, slot):
        sl = pl.ds(pl.multiple_of(t * QT, QT), QT)
        p = jnp.exp2(sref[...] - al[slot + 2]).astype(BF)
        acc[h, :, sl] = acc[h, :, sl] * al[slot] + jnp.dot(vscr[h], p, preferred_element_type=F32)

    def events(e):
        def at(k, fn):
            @pl.when(e == k)
            def _():
                fn()

        def hidden_next(j):
            if j == 1:
                h_dn[0].wait_recv()
                h_up[0].wait_recv()
                f_dn.start()
                h_mate[0].start()
                h_mate[1].start()
            elif j == 2:
                h_dn[1].wait_recv()
                h_up[1].wait_recv()
                f_up.start()
                h_mate[2].start()
                h_mate[3].start()
            else:
                f_dn.wait_recv()
                f_up.wait_recv()
                h_mate[4].start()
                h_mate[5].start()

        def w_step2():
            for t in range(2):
                w_arrived(t, 3, 0, 0, 32)
                w_arrived(t, 1, 0, 0, 32)
                for i in range(2):
                    w2[t, i].start()
                for d1 in (1, 3):
                    for i in range(2):
                        w3[t, d1, i].start()

        def w_step3():
            for t in range(2):
                w_arrived(t, 2, 0, 0, 16)
                w_arrived(t, 2, 0, 1, 16)
                w_arrived(t, 0, 1, 0, 32)
                w_arrived(t, 0, 3, 0, 32)
                for i in range(2):
                    w3[t, 2, i].start()
                for i in range(2):
                    w4[t, 0, i].start()
                for d in ((1, 0), (2, 0), (3, 0), (0, 1), (0, 3)):
                    w5[t, d[0], d[1]].start()

        def w_step4():
            for t in range(2):
                for d1 in (1, 3):
                    w_arrived(t, d1, 1, 0, 32)
                    w_arrived(t, d1, 3, 0, 32)
                    for i in range(2):
                        w4[t, d1, i].start()
                    w5[t, d1, 1].start()
                    w5[t, d1, 3].start()

        def w_step5():
            for t in range(2):
                w_arrived(t, 2, 1, 0, 32)
                w_arrived(t, 2, 3, 0, 32)
                for i in range(2):
                    w4[t, 2, i].start()
                w5[t, 2, 1].start()
                w5[t, 2, 3].start()
                w_arrived(t, 0, 2, 0, 16)
                w_arrived(t, 0, 2, 1, 16)
                w5[t, 0, 2].start()

        def w_step6():
            for t in range(2):
                for d1 in (1, 3, 2):
                    w_arrived(t, d1, 2, 0, 16)
                    w_arrived(t, d1, 2, 1, 16)
                    w5[t, d1, 2].start()

        at(2, w_step2)
        at(3, lambda: hidden_next(1))
        at(5, w_step3)
        at(7, lambda: hidden_next(2))
        at(9, w_step4)
        at(11, lambda: hidden_next(3))
        at(12, w_step5)
        at(15, w_step6)

    def chunk(j, carry):
        for k in range(1, 4):

            @pl.when(j == k)
            def _():
                h_mate[2 * k - 2].wait_recv()
                h_mate[2 * k - 1].wait_recv()

        edge = jnp.logical_or(j == 0, j == 3).astype(jnp.int32)
        for q in range(4):
            dz = edge * jnp.where(j == 0, 0, 2) + (1 - edge) * (1 if q < 2 else 3)
            cc = edge * (q // 2) + (1 - edge) * (q % 2)
            pp = edge * (q % 2) + (1 - edge) * (j - 1)
            base = (wrap(z + dz) * 2 + c + cc - 2 * c * cc) * 512 + pp * 256
            pos = lax.broadcasted_iota(jnp.int32, (256, 128), 0) + base
            bias = jnp.where(pos < length, 0.0, NEG).astype(BF)
            for pr_ in range(4):
                kscr[pr_, q * 256 : q * 256 + 256, 128:256] = bias
        xj = xbuf[j]
        for i in range(2):
            kk = jnp.dot(xj, wqkv[:, 512 + 256 * i : 768 + 256 * i], preferred_element_type=F32).astype(BF)
            kscr[2 * i, :, 0:128] = kk[:, 0:128]
            kscr[2 * i + 1, :, 0:128] = kk[:, 128:256]
            vt = jnp.dot(xj, wqkv[:, 1024 + 256 * i : 1280 + 256 * i], preferred_element_type=F32).T.astype(BF)
            for u in range(4):
                vscr[4 * i + u, 0:64, :] = vt[64 * u : 64 * u + 64]

        scores(0, 0, s_a, 0)

        def it(k, carry2):
            events(j * ITERS + k)
            for u in range(U):
                i = k * U + u
                nx = jnp.minimum(i + 1, TILES - 1)
                scores(nx // NT, lax.rem(nx, NT), bufs[(u + 1) % 2], (u + 1) % 2)
                values(i // NT, i % NT, bufs[u % 2], u % 2)
            return carry2

        lax.fori_loop(0, ITERS, it, 0)
        return carry

    lax.fori_loop(0, 4, chunk, 0)

    for pr_ in range(4):
        pair = []
        for h in (2 * pr_, 2 * pr_ + 1):
            pair.append(acc[h, 0:64, :] / acc[h, 64:65, :])
        both = jnp.concatenate(pair, axis=0)
        stage[:, 128 * pr_ : 128 * pr_ + 128] = both.T.astype(BF)
    my_cols = pl.ds(pl.multiple_of(c * 512, 512), 512)
    o_mate = rcopy(stage.at[pl.ds(512, 512)], att_ref.at[:, my_cols], osem.at[0], osem.at[1], mate)
    o_mine = pltpu.make_async_copy(stage.at[pl.ds(0, 512)], att_ref.at[:, my_cols], osem.at[2])
    o_mate.start()
    o_mine.start()
    for cp in w5.values():
        cp.wait()
    for group in (w1, w2, w3, w4):
        for cp in group.values():
            cp.wait_send()
    for cp in outs:
        cp.wait()
    for cp in h_dn + h_up + [f_dn, f_up, h_own] + h_mate:
        cp.wait_send()
    o_mine.wait()
    o_mate.wait()


def attend(length, tokens, project, up, down):
    any_spec = pl.BlockSpec(memory_space=pl.ANY)
    dma = pltpu.SemaphoreType.DMA
    return pl.pallas_call(
        attend_kernel,
        name="attend",
        out_shape=(
            jax.ShapeDtypeStruct((512, 1024), BF),
            jax.ShapeDtypeStruct((2, 1024, 4096), BF),
        ),
        in_specs=[pl.BlockSpec(memory_space=pltpu.SMEM)] + [any_spec] * 4,
        out_specs=(any_spec, any_spec),
        scratch_shapes=[
            pltpu.VMEM((4, 1024, 1024), BF),
            pltpu.VMEM((1024, 1536), BF),
            pltpu.VMEM((4, KB, 256), BF),
            pltpu.VMEM((8, 80, KB), BF),
            pltpu.VMEM((8, 256, 1024), BF),
            pltpu.VMEM((8, 80, 1024), F32),
            pltpu.VMEM((8, 1, 1024), F32),
            pltpu.VMEM((KB, QT), F32),
            pltpu.VMEM((KB, QT), F32),
            pltpu.VMEM((4, 1, QT), F32),
            pltpu.VMEM((1024, 512), BF),
            pltpu.VMEM((2, 64, 4096), BF),
            dma((8,)), dma((6,)), dma((6,)), dma((7,)), dma((7,)),
            dma((2, 20)), dma((2, 4, 4, 2)), dma((2, 4, 4)), dma((2, 4, 4)), dma((3,)),
        ],
        compiler_params=pltpu.CompilerParams(
            collective_id=0, has_side_effects=True, vmem_limit_bytes=62 * 2**20
        ),
    )(length, tokens, project, up, down)


def layer_norm(values, gain, shift):
    average = jnp.mean(values, axis=-1, keepdims=True)
    centred = values - average
    variance = jnp.mean(centred * centred, axis=-1, keepdims=True)
    return centred * lax.rsqrt(variance + 1e-05) * gain + shift


FC = 512
RB = 256


def feed_kernel(info_ref, att_ref, tok_ref, wo_ref, vec_ref, up_ref, dn_ref, out_ref, tot_ref, normed, acc):
    i = pl.program_id(0)

    @pl.when(i == 0)
    def _():
        for r in range(512 // RB):
            rows = pl.ds(r * RB, RB)
            mixed = jnp.dot(att_ref[rows, :], wo_ref[...], preferred_element_type=F32)
            mixed = mixed + tok_ref[rows, :].astype(F32)
            n = layer_norm(mixed, vec_ref[0:1, :], vec_ref[1:2, :]).astype(BF)
            normed[rows, :] = n
            acc[rows, :] = n.astype(F32)

    for r in range(512 // RB):
        rows = pl.ds(r * RB, RB)
        h = jnp.dot(normed[rows, :], up_ref[0], preferred_element_type=F32)
        inner = (0.5 * h * (1.0 + lax.erf(h * math.sqrt(0.5)))).astype(BF)
        acc[rows, :] += lax.dot_general(
            inner, dn_ref[0], (((1,), (1,)), ((), ())), preferred_element_type=F32
        )

    @pl.when(i == 4096 // FC - 1)
    def _():
        total = jnp.zeros((1, 1024), F32)
        for r in range(512 // RB):
            rows = pl.ds(r * RB, RB)
            final = layer_norm(acc[rows, :], vec_ref[2:3, :], vec_ref[3:4, :])
            out_ref[rows, :] = final.astype(BF)
            pos = lax.broadcasted_iota(jnp.int32, (RB, 1), 0) + (info_ref[1] + r * RB)
            valid = (pos < info_ref[0]).astype(F32)
            total = total + jnp.sum(final * valid, axis=0, keepdims=True)
        tot_ref[...] = total


def feed(info, att, tokens, output_weight, vecs, wf):
    whole = lambda shape: pl.BlockSpec(shape, lambda i: (0,) * len(shape))
    return pl.pallas_call(
        feed_kernel,
        name="feed",
        grid=(4096 // FC,),
        out_shape=(jax.ShapeDtypeStruct((512, 1024), BF), jax.ShapeDtypeStruct((1, 1024), F32)),
        in_specs=[
            pl.BlockSpec(memory_space=pltpu.SMEM),
            whole((512, 1024)),
            whole((512, 1024)),
            whole((1024, 1024)),
            whole((4, 1024)),
            pl.BlockSpec((1, 1024, FC), lambda i: (0, 0, i)),
            pl.BlockSpec((1, 1024, FC), lambda i: (1, 0, i)),
        ],
        out_specs=(whole((512, 1024)), whole((1, 1024))),
        scratch_shapes=[pltpu.VMEM((512, 1024), BF), pltpu.VMEM((512, 1024), F32)],
        compiler_params=pltpu.CompilerParams(
            dimension_semantics=("arbitrary",), vmem_limit_bytes=56 * 2**20
        ),
    )(info, att, tokens, output_weight, vecs, wf, wf)


def loss_kernel(len_ref, pos_ref, tot_ref, q_ref, emb_ref, loss_ref, parts, sent, passages, ssem, rsem, ssem2, rsem2):
    s = lax.axis_index("seq")
    g = lax.axis_index("grp")
    barrier = pltpu.get_barrier_semaphore()
    for d in range(1, 8):
        pl.semaphore_signal(barrier, inc=1, device_id={"seq": lax.rem(s + d, 8)}, device_id_type=MESH)
    for d in range(1, 16):
        pl.semaphore_signal(barrier, inc=1, device_id={"grp": lax.rem(g + d, 16)}, device_id_type=MESH)
    pl.semaphore_wait(barrier, 22)
    first = []
    for d in range(1, 8):
        cp = pltpu.make_async_remote_copy(
            src_ref=tot_ref, dst_ref=parts.at[d], send_sem=ssem.at[d], recv_sem=rsem.at[d],
            device_id={"seq": lax.rem(s + d, 8)}, device_id_type=MESH,
        )
        cp.start()
        first.append(cp)
    qv = q_ref[...]
    short_q = (qv / jnp.sqrt(jnp.sum(qv * qv, axis=-1, keepdims=True) + 1e-06)).astype(BF)
    for cp in first:
        cp.wait_recv()
    total = tot_ref[...]
    for d in range(1, 8):
        total = total + parts[d]
    pooled = total / len_ref[0].astype(F32)
    emb = pooled / jnp.sqrt(jnp.sum(pooled * pooled, axis=-1, keepdims=True) + 1e-06)
    emb_ref[...] = emb
    sent[...] = emb
    second = []
    for d in range(1, 16):
        cp = pltpu.make_async_remote_copy(
            src_ref=sent, dst_ref=passages.at[d], send_sem=ssem2.at[d], recv_sem=rsem2.at[d],
            device_id={"grp": lax.rem(g + d, 16)}, device_id_type=MESH,
        )
        cp.start()
        second.append(cp)
    for cp in second:
        cp.wait_recv()
    rows = [emb] + [passages[d] for d in range(1, 16)]
    allp = jnp.concatenate(rows, axis=0).astype(BF)
    logits = 20.0 * lax.dot_general(
        short_q, allp, (((1,), (1,)), ((), ())), preferred_element_type=F32
    )
    ids = lax.rem(g + 16 - lax.broadcasted_iota(jnp.int32, (8, 16), 1), 16)
    picked = jnp.sum(jnp.where(pos_ref[...] == ids, logits, 0.0), axis=1, keepdims=True)
    loss_ref[...] = jnp.log(jnp.sum(jnp.exp(logits), axis=1, keepdims=True)) - picked
    for cp in first + second:
        cp.wait_send()


def losses(length, positive, total, queries):
    vm = pl.BlockSpec(memory_space=pltpu.VMEM)
    dma = pltpu.SemaphoreType.DMA
    return pl.pallas_call(
        loss_kernel,
        name="losses",
        out_shape=(jax.ShapeDtypeStruct((1, 1024), F32), jax.ShapeDtypeStruct((8, 1), F32)),
        in_specs=[pl.BlockSpec(memory_space=pltpu.SMEM), vm, vm, vm],
        out_specs=(vm, vm),
        scratch_shapes=[
            pltpu.VMEM((8, 1, 1024), F32),
            pltpu.VMEM((1, 1024), F32),
            pltpu.VMEM((16, 1, 1024), F32),
            dma((8,)), dma((8,)), dma((16,)), dma((16,)),
        ],
        compiler_params=pltpu.CompilerParams(collective_id=1, has_side_effects=True),
    )(length, positive, total, queries)


def body(
    hidden_in, lengths, project_weight, output_weight, first_gain, first_shift,
    up_weight, down_weight, second_gain, second_shift, queries, positive,
):
    tokens = hidden_in[0]
    att, wf = attend(lengths, tokens, project_weight, up_weight, down_weight)
    vecs = jnp.stack([first_gain, first_shift, second_gain, second_shift])
    info = jnp.concatenate([lengths, (lax.axis_index("seq") * 512)[None].astype(jnp.int32)])
    final, total = feed(info, att, tokens, output_weight, vecs, wf)
    embedding, loss = losses(lengths, positive[:, None], total, queries)
    return final[None], embedding, loss[:, 0]


def solution(mesh):
    in_specs = (
        P("grp", "seq", None), P("grp"), P(), P(), P(), P(),
        P("grp", None), P("grp", None), P(), P(), P("grp", None), P("grp"),
    )
    out_specs = (P("grp", "seq", None), P("grp", None), P("grp"))
    return jax.shard_map(body, mesh=mesh, in_specs=in_specs, out_specs=out_specs, check_vma=False)
```

```python
import math
import functools

import jax
import jax.numpy as jnp
from jax import lax
from jax.experimental import pallas as pl
from jax.experimental.pallas import tpu as pltpu
from jax.sharding import PartitionSpec as P

MESH = pl.DeviceIdType.MESH
BF = jnp.bfloat16
F32 = jnp.float32
NEG = -1e30
KB = 1024
QT = 512
NT = 1024 // QT
TILES = 8 * NT
U = 4
ITERS = TILES // U
SCALE = math.log2(math.e) / 8.0


def attend_kernel(
    len_ref, x_ref, w_ref, up_ref, dn_ref, att_ref, wf_ref,
    xbuf, wqkv, kscr, vscr, qscr, acc, mx, s_a, s_b, al, stage, wv,
    lsem, hs, hr, ds, dr, ws, wr, ps, pr, osem,
):
    s = lax.axis_index("seq")
    g = lax.axis_index("grp")
    c = lax.rem(s, 2)
    z = s // 2
    gx = lax.rem(g, 4)
    gy = g // 4
    mate = {"seq": s + 1 - 2 * c}
    zup = {"seq": lax.rem(s + 2, 8)}
    zdn = {"seq": lax.rem(s + 6, 8)}

    def wrap(v):
        return lax.rem(v, 4)

    def peer(axis, step):
        if axis == 0:
            return {"grp": gy * 4 + wrap(gx + step)}
        return {"grp": wrap(gy + step) * 4 + gx}

    loads = [pltpu.make_async_copy(x_ref, xbuf.at[0, pl.ds(0, 512)], lsem.at[0])]
    for t in range(3):
        cols = pl.ds(pl.multiple_of(t * 1024 + c * 512, 512), 512)
        loads.append(
            pltpu.make_async_copy(w_ref.at[:, cols], wqkv.at[:, pl.ds(t * 512, 512)], lsem.at[1 + t])
        )
    loads.append(pltpu.make_async_copy(up_ref, wv.at[0], lsem.at[4]))
    loads.append(pltpu.make_async_copy(dn_ref, wv.at[1], lsem.at[5]))
    for cp in loads:
        cp.start()

    peers = [mate, zup, zdn, peer(0, 1), peer(0, 3), peer(1, 1), peer(1, 3)]
    barrier = pltpu.get_barrier_semaphore()
    for d in peers:
        pl.semaphore_signal(barrier, inc=1, device_id=d, device_id_type=MESH)
    pl.semaphore_wait(barrier, len(peers))

    def rcopy(src, dst, ssem, rsem, dev):
        return pltpu.make_async_remote_copy(
            src_ref=src, dst_ref=dst, send_sem=ssem, recv_sem=rsem, device_id=dev, device_id_type=MESH
        )

    def h_piece(p):
        return xbuf.at[0, pl.ds(p * 256, 256)]

    def x_quarter(j, q):
        return xbuf.at[j, pl.ds(q * 256, 256)]

    h_own = rcopy(xbuf.at[0, pl.ds(0, 512)], xbuf.at[0, pl.ds(512, 512)], ds.at[0], dr.at[0], mate)
    h_dn = [rcopy(h_piece(p), x_quarter(1 + p, 0), hs.at[p], hr.at[p], zdn) for p in range(2)]
    h_up = [rcopy(h_piece(p), x_quarter(1 + p, 2), hs.at[2 + p], hr.at[2 + p], zup) for p in range(2)]
    f_dn = rcopy(x_quarter(1, 0), x_quarter(3, 0), hs.at[4], hr.at[4], zdn)
    f_up = rcopy(x_quarter(2, 2), x_quarter(3, 1), hs.at[5], hr.at[5], zup)
    h_mate = []
    for k, (j, a, b) in enumerate([(1, 0, 1), (1, 2, 3), (2, 0, 1), (2, 2, 3), (3, 0, 2), (3, 1, 3)]):
        h_mate.append(rcopy(x_quarter(j, a), x_quarter(j, b), ds.at[1 + k], dr.at[1 + k], mate))

    def origin_row(t, d1, d2):
        dx, dy = (d1, d2) if t == 0 else (d2, d1)
        return (wrap(gy + dy) * 4 + wrap(gx + dx)) * 64 + t * 32

    def w_reg(t, d1, d2, lo, n):
        return wf_ref.at[c, pl.ds(pl.multiple_of(origin_row(t, d1, d2) + lo, 16), n), :]

    w1, w2, w3, w4 = {}, {}, {}, {}
    for t in range(2):
        mine = wv.at[c, pl.ds(t * 32, 32), :]
        a1, a2 = t, 1 - t
        for i, (step, seen) in enumerate([(1, 3), (3, 1)]):
            w1[t, i] = rcopy(mine, w_reg(t, 0, 0, 0, 32), ws.at[t, i], wr.at[t, seen, 0, 0], peer(a1, step))
            w2[t, i] = rcopy(
                w_reg(t, seen, 0, 16 * i, 16), w_reg(t, seen, 0, 16 * i, 16),
                ws.at[t, 2 + i], wr.at[t, 2, 0, i], peer(a1, step),
            )
            for d1 in range(4):
                src = mine if d1 == 0 else w_reg(t, d1, 0, 0, 32)
                w3[t, d1, i] = rcopy(
                    src, w_reg(t, d1, 0, 0, 32), ws.at[t, 4 + 2 * d1 + i], wr.at[t, d1, seen, 0], peer(a2, step)
                )
                w4[t, d1, i] = rcopy(
                    w_reg(t, d1, seen, 16 * i, 16), w_reg(t, d1, seen, 16 * i, 16),
                    ws.at[t, 12 + 2 * d1 + i], wr.at[t, d1, 2, i], peer(a2, step),
                )
    w5 = {}
    for t in range(2):
        for d1 in range(4):
            for d2 in range(4):
                if d1 or d2:
                    w5[t, d1, d2] = rcopy(
                        w_reg(t, d1, d2, 0, 32), w_reg(t, d1, d2, 0, 32),
                        ps.at[t, d1, d2], pr.at[t, d1, d2], mate,
                    )

    def w_arrived(t, d1, d2, k, n):
        reg = w_reg(t, d1, d2, 16 * k, n)
        pltpu.make_async_copy(reg, reg, wr.at[t, d1, d2, k]).wait()

    loads[0].wait()
    for cp in h_dn + h_up + [h_own]:
        cp.start()
    loads[4].wait()
    loads[5].wait()
    for t in range(2):
        for i in range(2):
            w1[t, i].start()
    for t in range(2):
        for i in range(2):
            w3[t, 0, i].start()
    own_rows = pl.ds(pl.multiple_of(g * 64, 64), 64)
    outs = [pltpu.make_async_copy(wv.at[k], wf_ref.at[k, own_rows, :], lsem.at[6 + k]) for k in range(2)]
    for cp in outs:
        cp.start()

    qscr[...] = jnp.zeros_like(qscr)
    for h in range(8):
        qscr[h, 128:144, :] = (lax.broadcasted_iota(jnp.int32, (16, KB), 0) == 0).astype(BF)
        vscr[h, 64:80, :] = jnp.ones((16, KB), BF)
    acc[...] = jnp.zeros_like(acc)
    mx[...] = jnp.full_like(mx, NEG)
    length = len_ref[0]

    for k in range(3):
        loads[1 + k].wait()
    h_own.wait_recv()
    for i in range(2):
        q = jnp.dot(xbuf[0], wqkv[:, 256 * i : 256 * i + 256], preferred_element_type=F32)
        qt = (q * SCALE).T.astype(BF)
        for u in range(4):
            h = 4 * i + u
            qscr[h, (u % 2) * 64 : (u % 2) * 64 + 64, :] = qt[64 * u : 64 * u + 64]

    bufs = [s_a, s_b]

    def scores(h, t, sref, slot):
        sl = pl.ds(pl.multiple_of(t * QT, QT), QT)
        sc = jnp.dot(kscr[h // 2], qscr[h, :, sl], preferred_element_type=F32)
        sref[...] = sc
        old = mx[h, :, sl]
        new = jnp.maximum(old, jnp.max(sc, axis=0, keepdims=True))
        mx[h, :, sl] = new
        al[slot] = jnp.exp2(old - new)
        al[slot + 2] = new

    def values(h, t, sref, slot):
        sl = pl.ds(pl.multiple_of(t * QT, QT), QT)
        p = jnp.exp2(sref[...] - al[slot + 2]).astype(BF)
        acc[h, :, sl] = acc[h, :, sl] * al[slot] + jnp.dot(vscr[h], p, preferred_element_type=F32)

    def events(e):
        def at(k, fn):
            @pl.when(e == k)
            def _():
                fn()

        def hidden_next(j):
            if j == 1:
                h_dn[0].wait_recv()
                h_up[0].wait_recv()
                f_dn.start()
                h_mate[0].start()
                h_mate[1].start()
            elif j == 2:
                h_dn[1].wait_recv()
                h_up[1].wait_recv()
                f_up.start()
                h_mate[2].start()
                h_mate[3].start()
            else:
                f_dn.wait_recv()
                f_up.wait_recv()
                h_mate[4].start()
                h_mate[5].start()

        def arrived(*blocks):
            for t in range(2):
                for d1, d2 in blocks:
                    if d1 == 2 and d2 == 0 or d2 == 2:
                        w_arrived(t, d1, d2, 0, 16)
                        w_arrived(t, d1, d2, 1, 16)
                    else:
                        w_arrived(t, d1, d2, 0, 32)

        def send(group, *d1s):
            for t in range(2):
                for i in range(2):
                    if d1s:
                        for d1 in d1s:
                            group[t, d1, i].start()
                    else:
                        group[t, i].start()

        def share(*blocks):
            for t in range(2):
                for d1, d2 in blocks:
                    w5[t, d1, d2].start()

        def e1():
            arrived((1, 0), (3, 0))
            send(w2)

        def e3():
            hidden_next(1)
            share((1, 0), (3, 0))

        def e5():
            arrived((0, 1), (0, 3))
            send(w4, 0)
            share((0, 1), (0, 3))

        def e6():
            arrived((2, 0))
            send(w3, 2)
            share((2, 0))

        def e8():
            arrived((1, 1), (1, 3))
            send(w4, 1)
            share((1, 1), (1, 3))

        def e9():
            arrived((3, 1), (3, 3))
            send(w4, 3)
            share((3, 1), (3, 3))

        def e10():
            arrived((0, 2))
            share((0, 2))

        def e11():
            hidden_next(3)
            arrived((2, 1), (2, 3))
            send(w4, 2)
            share((2, 1), (2, 3))

        def last(d1):
            arrived((d1, 2))
            share((d1, 2))

        at(1, e1)
        at(2, lambda: send(w3, 1))
        at(3, e3)
        at(4, lambda: send(w3, 3))
        at(5, e5)
        at(6, e6)
        at(7, lambda: hidden_next(2))
        at(8, e8)
        at(9, e9)
        at(10, e10)
        at(11, e11)
        at(12, lambda: last(1))
        at(13, lambda: last(3))
        at(14, lambda: last(2))

    def chunk(j, carry):
        for k in range(1, 4):

            @pl.when(j == k)
            def _():
                h_mate[2 * k - 2].wait_recv()
                h_mate[2 * k - 1].wait_recv()

        edge = jnp.logical_or(j == 0, j == 3).astype(jnp.int32)
        for q in range(4):
            dz = edge * jnp.where(j == 0, 0, 2) + (1 - edge) * (1 if q < 2 else 3)
            cc = edge * (q // 2) + (1 - edge) * (q % 2)
            pp = edge * (q % 2) + (1 - edge) * (j - 1)
            base = (wrap(z + dz) * 2 + c + cc - 2 * c * cc) * 512 + pp * 256
            pos = lax.broadcasted_iota(jnp.int32, (256, 128), 0) + base
            bias = jnp.where(pos < length, 0.0, NEG).astype(BF)
            for pr_ in range(4):
                kscr[pr_, q * 256 : q * 256 + 256, 128:256] = bias
        xj = xbuf[j]
        for i in range(2):
            kk = jnp.dot(xj, wqkv[:, 512 + 256 * i : 768 + 256 * i], preferred_element_type=F32).astype(BF)
            kscr[2 * i, :, 0:128] = kk[:, 0:128]
            kscr[2 * i + 1, :, 0:128] = kk[:, 128:256]
            vt = jnp.dot(xj, wqkv[:, 1024 + 256 * i : 1280 + 256 * i], preferred_element_type=F32).T.astype(BF)
            for u in range(4):
                vscr[4 * i + u, 0:64, :] = vt[64 * u : 64 * u + 64]

        scores(0, 0, s_a, 0)

        def it(k, carry2):
            events(j * ITERS + k)
            for u in range(U):
                i = k * U + u
                nx = jnp.minimum(i + 1, TILES - 1)
                scores(nx // NT, lax.rem(nx, NT), bufs[(u + 1) % 2], (u + 1) % 2)
                values(i // NT, i % NT, bufs[u % 2], u % 2)
            return carry2

        lax.fori_loop(0, ITERS, it, 0)
        return carry

    lax.fori_loop(0, 4, chunk, 0)

    for pr_ in range(4):
        pair = []
        for h in (2 * pr_, 2 * pr_ + 1):
            pair.append(acc[h, 0:64, :] / acc[h, 64:65, :])
        both = jnp.concatenate(pair, axis=0)
        stage[:, 128 * pr_ : 128 * pr_ + 128] = both.T.astype(BF)
    my_cols = pl.ds(pl.multiple_of(c * 512, 512), 512)
    o_mate = rcopy(stage.at[pl.ds(512, 512)], att_ref.at[:, my_cols], osem.at[0], osem.at[1], mate)
    o_mine = pltpu.make_async_copy(stage.at[pl.ds(0, 512)], att_ref.at[:, my_cols], osem.at[2])
    o_mate.start()
    o_mine.start()
    for cp in w5.values():
        cp.wait()
    for group in (w1, w2, w3, w4):
        for cp in group.values():
            cp.wait_send()
    for cp in outs:
        cp.wait()
    for cp in h_dn + h_up + [f_dn, f_up, h_own] + h_mate:
        cp.wait_send()
    o_mine.wait()
    o_mate.wait()


def attend(length, tokens, project, up, down):
    any_spec = pl.BlockSpec(memory_space=pl.ANY)
    dma = pltpu.SemaphoreType.DMA
    return pl.pallas_call(
        attend_kernel,
        name="attend",
        out_shape=(
            jax.ShapeDtypeStruct((512, 1024), BF),
            jax.ShapeDtypeStruct((2, 1024, 4096), BF),
        ),
        in_specs=[pl.BlockSpec(memory_space=pltpu.SMEM)] + [any_spec] * 4,
        out_specs=(any_spec, any_spec),
        scratch_shapes=[
            pltpu.VMEM((4, 1024, 1024), BF),
            pltpu.VMEM((1024, 1536), BF),
            pltpu.VMEM((4, KB, 256), BF),
            pltpu.VMEM((8, 80, KB), BF),
            pltpu.VMEM((8, 256, 1024), BF),
            pltpu.VMEM((8, 80, 1024), F32),
            pltpu.VMEM((8, 1, 1024), F32),
            pltpu.VMEM((KB, QT), F32),
            pltpu.VMEM((KB, QT), F32),
            pltpu.VMEM((4, 1, QT), F32),
            pltpu.VMEM((1024, 512), BF),
            pltpu.VMEM((2, 64, 4096), BF),
            dma((8,)), dma((6,)), dma((6,)), dma((7,)), dma((7,)),
            dma((2, 20)), dma((2, 4, 4, 2)), dma((2, 4, 4)), dma((2, 4, 4)), dma((3,)),
        ],
        compiler_params=pltpu.CompilerParams(
            collective_id=0, has_side_effects=True, vmem_limit_bytes=62 * 2**20
        ),
    )(length, tokens, project, up, down)


def layer_norm(values, gain, shift):
    average = jnp.mean(values, axis=-1, keepdims=True)
    centred = values - average
    variance = jnp.mean(centred * centred, axis=-1, keepdims=True)
    return centred * lax.rsqrt(variance + 1e-05) * gain + shift


FC = 1024
RB = 512


def feed_kernel(
    len_ref, att_ref, tok_ref, wo_ref, g1_ref, b1_ref, g2_ref, b2_ref, up_ref, dn_ref, out_ref, tot_ref, normed, acc
):
    i = pl.program_id(0)

    @pl.when(i == 0)
    def _():
        for r in range(512 // RB):
            rows = pl.ds(r * RB, RB)
            mixed = jnp.dot(att_ref[rows, :], wo_ref[...], preferred_element_type=F32)
            mixed = mixed + tok_ref[rows, :].astype(F32)
            n = layer_norm(mixed, g1_ref[...], b1_ref[...]).astype(BF)
            normed[rows, :] = n
            acc[rows, :] = n.astype(F32)

    for r in range(512 // RB):
        rows = pl.ds(r * RB, RB)
        h = jnp.dot(normed[rows, :], up_ref[0], preferred_element_type=F32)
        inner = (0.5 * h * (1.0 + lax.erf(h * math.sqrt(0.5)))).astype(BF)
        acc[rows, :] += lax.dot_general(
            inner, dn_ref[0], (((1,), (1,)), ((), ())), preferred_element_type=F32
        )

    @pl.when(i == 4096 // FC - 1)
    def _():
        total = jnp.zeros((1, 1024), F32)
        for r in range(512 // RB):
            rows = pl.ds(r * RB, RB)
            final = layer_norm(acc[rows, :], g2_ref[...], b2_ref[...])
            out_ref[rows, :] = final.astype(BF)
            pos = lax.broadcasted_iota(jnp.int32, (RB, 1), 0) + (lax.axis_index("seq") * 512 + r * RB)
            valid = (pos < len_ref[0]).astype(F32)
            total = total + jnp.sum(final * valid, axis=0, keepdims=True)
        tot_ref[...] = total


def feed(lengths, att, tokens, output_weight, rows, wf):
    whole = lambda shape: pl.BlockSpec(shape, lambda i: (0,) * len(shape))
    return pl.pallas_call(
        feed_kernel,
        name="feed",
        grid=(4096 // FC,),
        out_shape=(jax.ShapeDtypeStruct((512, 1024), BF), jax.ShapeDtypeStruct((1, 1024), F32)),
        in_specs=[
            pl.BlockSpec(memory_space=pltpu.SMEM),
            whole((512, 1024)),
            whole((512, 1024)),
            whole((1024, 1024)),
            *[whole((1, 1024))] * 4,
            pl.BlockSpec((1, 1024, FC), lambda i: (0, 0, i)),
            pl.BlockSpec((1, 1024, FC), lambda i: (1, 0, i)),
        ],
        out_specs=(whole((512, 1024)), whole((1, 1024))),
        scratch_shapes=[pltpu.VMEM((512, 1024), BF), pltpu.VMEM((512, 1024), F32)],
        compiler_params=pltpu.CompilerParams(
            dimension_semantics=("arbitrary",), vmem_limit_bytes=56 * 2**20
        ),
    )(lengths, att, tokens, output_weight, *rows, wf, wf)


def loss_kernel(len_ref, pos_ref, tot_ref, q_ref, emb_ref, loss_ref, parts, sent, passages, ssem, rsem, ssem2, rsem2):
    s = lax.axis_index("seq")
    g = lax.axis_index("grp")
    barrier = pltpu.get_barrier_semaphore()
    for d in range(1, 8):
        pl.semaphore_signal(barrier, inc=1, device_id={"seq": lax.rem(s + d, 8)}, device_id_type=MESH)
    for d in range(1, 16):
        pl.semaphore_signal(barrier, inc=1, device_id={"grp": lax.rem(g + d, 16)}, device_id_type=MESH)
    pl.semaphore_wait(barrier, 22)
    first = []
    for d in range(1, 8):
        cp = pltpu.make_async_remote_copy(
            src_ref=tot_ref, dst_ref=parts.at[d], send_sem=ssem.at[d], recv_sem=rsem.at[d],
            device_id={"seq": lax.rem(s + d, 8)}, device_id_type=MESH,
        )
        cp.start()
        first.append(cp)
    qv = q_ref[...]
    short_q = (qv / jnp.sqrt(jnp.sum(qv * qv, axis=-1, keepdims=True) + 1e-06)).astype(BF)
    for cp in first:
        cp.wait_recv()
    total = tot_ref[...]
    for d in range(1, 8):
        total = total + parts[d]
    pooled = total / len_ref[0].astype(F32)
    emb = pooled / jnp.sqrt(jnp.sum(pooled * pooled, axis=-1, keepdims=True) + 1e-06)
    emb_ref[...] = emb
    sent[...] = emb
    second = []
    for d in range(1, 16):
        cp = pltpu.make_async_remote_copy(
            src_ref=sent, dst_ref=passages.at[d], send_sem=ssem2.at[d], recv_sem=rsem2.at[d],
            device_id={"grp": lax.rem(g + d, 16)}, device_id_type=MESH,
        )
        cp.start()
        second.append(cp)
    for cp in second:
        cp.wait_recv()
    rows = [emb] + [passages[d] for d in range(1, 16)]
    allp = jnp.concatenate(rows, axis=0).astype(BF)
    logits = 20.0 * lax.dot_general(
        allp, short_q, (((1,), (1,)), ((), ())), preferred_element_type=F32
    )
    ids = lax.rem(g + 16 - lax.broadcasted_iota(jnp.int32, (16, 8), 0), 16)
    picked = jnp.sum(jnp.where(pos_ref[...] == ids, logits, 0.0), axis=0, keepdims=True)
    loss_ref[...] = jnp.log(jnp.sum(jnp.exp(logits), axis=0, keepdims=True)) - picked
    for cp in first + second:
        cp.wait_send()


def losses(length, positive, total, queries):
    vm = pl.BlockSpec(memory_space=pltpu.VMEM)
    dma = pltpu.SemaphoreType.DMA
    return pl.pallas_call(
        loss_kernel,
        name="losses",
        out_shape=(jax.ShapeDtypeStruct((1, 1024), F32), jax.ShapeDtypeStruct((1, 8), F32)),
        in_specs=[pl.BlockSpec(memory_space=pltpu.SMEM), vm, vm, vm],
        out_specs=(vm, vm),
        scratch_shapes=[
            pltpu.VMEM((8, 1, 1024), F32),
            pltpu.VMEM((1, 1024), F32),
            pltpu.VMEM((16, 1, 1024), F32),
            dma((8,)), dma((8,)), dma((16,)), dma((16,)),
        ],
        compiler_params=pltpu.CompilerParams(collective_id=1, has_side_effects=True),
    )(length, positive, total, queries)


def body(
    hidden_in, lengths, project_weight, output_weight, first_gain, first_shift,
    up_weight, down_weight, second_gain, second_shift, queries, positive,
):
    tokens = hidden_in[0]
    att, wf = attend(lengths, tokens, project_weight, up_weight, down_weight)
    rows = [v[None, :] for v in (first_gain, first_shift, second_gain, second_shift)]
    final, total = feed(lengths, att, tokens, output_weight, rows, wf)
    embedding, loss = losses(lengths, positive[None, :], total, queries)
    return final[None], embedding, loss[0]


def solution(mesh):
    in_specs = (
        P("grp", "seq", None), P("grp"), P(), P(), P(), P(),
        P("grp", None), P("grp", None), P(), P(), P("grp", None), P("grp"),
    )
    out_specs = (P("grp", "seq", None), P("grp", None), P("grp"))
    return jax.shard_map(body, mesh=mesh, in_specs=in_specs, out_specs=out_specs, check_vma=False)
```

```python
import math
import functools

import jax
import jax.numpy as jnp
from jax import lax
from jax.experimental import pallas as pl
from jax.experimental.pallas import tpu as pltpu
from jax.sharding import PartitionSpec as P

MESH = pl.DeviceIdType.MESH
BF = jnp.bfloat16
F32 = jnp.float32
NEG = -1e30
KB = 1024
RS = 256
EV = (3, 3, 6, 6, 14, 14, 14, 18, 18, 22, 25, 28, 28, 30)
SCALE = math.log2(math.e) / 8.0


def attend_kernel(
    len_ref, x_ref, w_ref, up_ref, dn_ref, att_ref, wf_ref,
    xbuf, wqkv, kscr, vscr, qscr, acc, mx, sbuf, al, stage, wv,
    lsem, hs, hr, ds, dr, ws, wr, ps, pr, osem,
):
    s = lax.axis_index("seq")
    g = lax.axis_index("grp")
    c = lax.rem(s, 2)
    z = s // 2
    gx = lax.rem(g, 4)
    gy = g // 4
    mate = {"seq": s + 1 - 2 * c}
    zup = {"seq": lax.rem(s + 2, 8)}
    zdn = {"seq": lax.rem(s + 6, 8)}

    def wrap(v):
        return lax.rem(v, 4)

    def peer(axis, step):
        if axis == 0:
            return {"grp": gy * 4 + wrap(gx + step)}
        return {"grp": wrap(gy + step) * 4 + gx}

    loads = [pltpu.make_async_copy(x_ref, xbuf.at[0, pl.ds(0, 512)], lsem.at[0])]
    for t in range(3):
        cols = pl.ds(pl.multiple_of(t * 1024 + c * 512, 512), 512)
        loads.append(
            pltpu.make_async_copy(w_ref.at[:, cols], wqkv.at[:, pl.ds(t * 512, 512)], lsem.at[1 + t])
        )
    loads.append(pltpu.make_async_copy(up_ref, wv.at[0], lsem.at[4]))
    loads.append(pltpu.make_async_copy(dn_ref, wv.at[1], lsem.at[5]))
    for cp in loads:
        cp.start()

    peers = [mate, zup, zdn, peer(0, 1), peer(0, 3), peer(1, 1), peer(1, 3)]
    barrier = pltpu.get_barrier_semaphore()
    for d in peers:
        pl.semaphore_signal(barrier, inc=1, device_id=d, device_id_type=MESH)
    pl.semaphore_wait(barrier, len(peers))

    def rcopy(src, dst, ssem, rsem, dev):
        return pltpu.make_async_remote_copy(
            src_ref=src, dst_ref=dst, send_sem=ssem, recv_sem=rsem, device_id=dev, device_id_type=MESH
        )

    def h_piece(p):
        return xbuf.at[0, pl.ds(p * 256, 256)]

    def x_quarter(j, q):
        return xbuf.at[j, pl.ds(q * 256, 256)]

    h_own = rcopy(xbuf.at[0, pl.ds(0, 512)], xbuf.at[0, pl.ds(512, 512)], ds.at[0], dr.at[0], mate)
    h_dn = [rcopy(h_piece(p), x_quarter(1 + p, 0), hs.at[p], hr.at[p], zdn) for p in range(2)]
    h_up = [rcopy(h_piece(p), x_quarter(1 + p, 2), hs.at[2 + p], hr.at[2 + p], zup) for p in range(2)]
    f_dn = rcopy(x_quarter(1, 0), x_quarter(3, 0), hs.at[4], hr.at[4], zdn)
    f_up = rcopy(x_quarter(2, 2), x_quarter(3, 1), hs.at[5], hr.at[5], zup)
    h_mate = []
    for k, (j, a, b) in enumerate([(1, 0, 1), (1, 2, 3), (2, 0, 1), (2, 2, 3), (3, 0, 2), (3, 1, 3)]):
        h_mate.append(rcopy(x_quarter(j, a), x_quarter(j, b), ds.at[1 + k], dr.at[1 + k], mate))

    def origin_row(t, d1, d2):
        dx, dy = (d1, d2) if t == 0 else (d2, d1)
        return (wrap(gy + dy) * 4 + wrap(gx + dx)) * 64 + t * 32

    def w_reg(t, d1, d2, lo, n):
        return wf_ref.at[c, pl.ds(pl.multiple_of(origin_row(t, d1, d2) + lo, 16), n), :]

    w1, w2, w3, w4 = {}, {}, {}, {}
    for t in range(2):
        mine = wv.at[c, pl.ds(t * 32, 32), :]
        a1, a2 = t, 1 - t
        for i, (step, seen) in enumerate([(1, 3), (3, 1)]):
            w1[t, i] = rcopy(mine, w_reg(t, 0, 0, 0, 32), ws.at[t, i], wr.at[t, seen, 0, 0], peer(a1, step))
            w2[t, i] = rcopy(
                w_reg(t, seen, 0, 16 * i, 16), w_reg(t, seen, 0, 16 * i, 16),
                ws.at[t, 2 + i], wr.at[t, 2, 0, i], peer(a1, step),
            )
            for d1 in range(4):
                src = mine if d1 == 0 else w_reg(t, d1, 0, 0, 32)
                w3[t, d1, i] = rcopy(
                    src, w_reg(t, d1, 0, 0, 32), ws.at[t, 4 + 2 * d1 + i], wr.at[t, d1, seen, 0], peer(a2, step)
                )
                w4[t, d1, i] = rcopy(
                    w_reg(t, d1, seen, 16 * i, 16), w_reg(t, d1, seen, 16 * i, 16),
                    ws.at[t, 12 + 2 * d1 + i], wr.at[t, d1, 2, i], peer(a2, step),
                )
    w5 = {}
    for t in range(2):
        for d1 in range(4):
            for d2 in range(4):
                if d1 or d2:
                    w5[t, d1, d2] = rcopy(
                        w_reg(t, d1, d2, 0, 32), w_reg(t, d1, d2, 0, 32),
                        ps.at[t, d1, d2], pr.at[t, d1, d2], mate,
                    )

    def w_arrived(t, d1, d2, k, n):
        reg = w_reg(t, d1, d2, 16 * k, n)
        pltpu.make_async_copy(reg, reg, wr.at[t, d1, d2, k]).wait()

    loads[0].wait()
    for cp in h_dn + h_up + [h_own]:
        cp.start()
    loads[4].wait()
    loads[5].wait()
    for t in range(2):
        for i in range(2):
            w1[t, i].start()
    for t in range(2):
        for i in range(2):
            w3[t, 0, i].start()
    own_rows = pl.ds(pl.multiple_of(g * 64, 64), 64)
    outs = [pltpu.make_async_copy(wv.at[k], wf_ref.at[k, own_rows, :], lsem.at[6 + k]) for k in range(2)]
    for cp in outs:
        cp.start()

    qscr[...] = jnp.zeros_like(qscr)
    for h in range(8):
        qscr[h, 128:144, :] = (lax.broadcasted_iota(jnp.int32, (16, KB), 0) == 0).astype(BF)
        vscr[h, 64:80, :] = jnp.ones((16, KB), BF)
    acc[...] = jnp.zeros_like(acc)
    mx[...] = jnp.full_like(mx, NEG)
    length = len_ref[0]

    for k in range(3):
        loads[1 + k].wait()
    h_own.wait_recv()
    for i in range(2):
        q = jnp.dot(xbuf[0], wqkv[:, 256 * i : 256 * i + 256], preferred_element_type=F32)
        qt = (q * SCALE).T.astype(BF)
        for u in range(4):
            h = 4 * i + u
            qscr[h, (u % 2) * 64 : (u % 2) * 64 + 64, :] = qt[64 * u : 64 * u + 64]

    def score_rows(h, r):
        rows = pl.ds(r * RS, RS)
        sc = jnp.dot(kscr[h // 2, rows, :], qscr[h], preferred_element_type=F32)
        sbuf[rows, :] = sc
        return jnp.max(sc.reshape(RS // 8, 8, 1024), axis=0)

    def new_max(h, tops):
        top = functools.reduce(jnp.maximum, tops)
        old = mx[h]
        new = jnp.maximum(old, jnp.max(top, axis=0, keepdims=True))
        mx[h] = new
        al[0] = jnp.exp2(old - new)
        al[1] = new

    def head_step(h, following):
        factor = al[0]
        top = al[1]
        tops = []
        out = None
        for r in range(KB // RS):
            p = jnp.exp2(sbuf[pl.ds(r * RS, RS), :] - top).astype(BF)
            if following is not None:
                tops.append(score_rows(following, r))
            part = jnp.dot(vscr[h, :, pl.ds(r * RS, RS)], p, preferred_element_type=F32)
            out = part if out is None else out + part
        if following is not None:
            new_max(following, tops)
        acc[h] = acc[h] * factor + out

    def events(e):
        def at(k, fn):
            @pl.when(e == k)
            def _():
                fn()

        def hidden_next(j):
            if j == 1:
                h_dn[0].wait_recv()
                h_up[0].wait_recv()
                f_dn.start()
                h_mate[0].start()
                h_mate[1].start()
            elif j == 2:
                h_dn[1].wait_recv()
                h_up[1].wait_recv()
                f_up.start()
                h_mate[2].start()
                h_mate[3].start()
            else:
                f_dn.wait_recv()
                f_up.wait_recv()
                h_mate[4].start()
                h_mate[5].start()

        def arrived(*blocks):
            for t in range(2):
                for d1, d2 in blocks:
                    if d1 == 2 and d2 == 0 or d2 == 2:
                        w_arrived(t, d1, d2, 0, 16)
                        w_arrived(t, d1, d2, 1, 16)
                    else:
                        w_arrived(t, d1, d2, 0, 32)

        def send(group, *d1s):
            for t in range(2):
                for i in range(2):
                    if d1s:
                        for d1 in d1s:
                            group[t, d1, i].start()
                    else:
                        group[t, i].start()

        def share(*blocks):
            for t in range(2):
                for d1, d2 in blocks:
                    w5[t, d1, d2].start()

        def e1():
            arrived((1, 0), (3, 0))
            send(w2)

        def e3():
            share((1, 0), (3, 0))

        def e5():
            arrived((0, 1), (0, 3))
            send(w4, 0)
            share((0, 1), (0, 3))

        def e6():
            arrived((2, 0))
            send(w3, 2)
            share((2, 0))

        def e8():
            arrived((1, 1), (1, 3))
            send(w4, 1)
            share((1, 1), (1, 3))

        def e9():
            arrived((3, 1), (3, 3))
            send(w4, 3)
            share((3, 1), (3, 3))

        def e10():
            arrived((0, 2))
            share((0, 2))

        def e11():
            arrived((2, 1), (2, 3))
            send(w4, 2)
            share((2, 1), (2, 3))

        def last(d1):
            arrived((d1, 2))
            share((d1, 2))

        at(EV[0], e1)
        at(EV[1], lambda: send(w3, 1))
        at(EV[2], e3)
        at(EV[3], lambda: send(w3, 3))
        at(EV[4], e5)
        at(EV[5], e6)
        at(12, lambda: hidden_next(2))
        at(5, lambda: hidden_next(1))
        at(20, lambda: hidden_next(3))
        at(EV[7], e8)
        at(EV[8], e9)
        at(EV[9], e10)
        at(EV[10], e11)
        at(EV[11], lambda: last(1))
        at(EV[12], lambda: last(3))
        at(EV[13], lambda: last(2))

    def chunk(j, carry):
        for k in range(1, 4):

            @pl.when(j == k)
            def _():
                h_mate[2 * k - 2].wait_recv()
                h_mate[2 * k - 1].wait_recv()

        edge = jnp.logical_or(j == 0, j == 3).astype(jnp.int32)
        for q in range(4):
            dz = edge * jnp.where(j == 0, 0, 2) + (1 - edge) * (1 if q < 2 else 3)
            cc = edge * (q // 2) + (1 - edge) * (q % 2)
            pp = edge * (q % 2) + (1 - edge) * (j - 1)
            base = (wrap(z + dz) * 2 + c + cc - 2 * c * cc) * 512 + pp * 256
            pos = lax.broadcasted_iota(jnp.int32, (256, 128), 0) + base
            bias = jnp.where(pos < length, 0.0, NEG).astype(BF)
            for pr_ in range(4):
                kscr[pr_, q * 256 : q * 256 + 256, 128:256] = bias
        xj = xbuf[j]
        for i in range(2):
            kk = jnp.dot(xj, wqkv[:, 512 + 256 * i : 768 + 256 * i], preferred_element_type=F32).astype(BF)
            kscr[2 * i, :, 0:128] = kk[:, 0:128]
            kscr[2 * i + 1, :, 0:128] = kk[:, 128:256]
            vt = jnp.dot(xj, wqkv[:, 1024 + 256 * i : 1280 + 256 * i], preferred_element_type=F32).T.astype(BF)
            for u in range(4):
                vscr[4 * i + u, 0:64, :] = vt[64 * u : 64 * u + 64]

        new_max(0, [score_rows(0, r) for r in range(KB // RS)])

        def it(h, carry2):
            events(j * 8 + h)
            head_step(h, h + 1)
            return carry2

        lax.fori_loop(0, 7, it, 0)
        head_step(7, None)
        return carry

    lax.fori_loop(0, 4, chunk, 0)

    for pr_ in range(4):
        pair = []
        for h in (2 * pr_, 2 * pr_ + 1):
            pair.append(acc[h, 0:64, :] / acc[h, 64:65, :])
        both = jnp.concatenate(pair, axis=0)
        stage[:, 128 * pr_ : 128 * pr_ + 128] = both.T.astype(BF)
    my_cols = pl.ds(pl.multiple_of(c * 512, 512), 512)
    o_mate = rcopy(stage.at[pl.ds(512, 512)], att_ref.at[:, my_cols], osem.at[0], osem.at[1], mate)
    o_mine = pltpu.make_async_copy(stage.at[pl.ds(0, 512)], att_ref.at[:, my_cols], osem.at[2])
    o_mate.start()
    o_mine.start()
    for cp in w5.values():
        cp.wait()
    for group in (w1, w2, w3, w4):
        for cp in group.values():
            cp.wait_send()
    for cp in outs:
        cp.wait()
    for cp in h_dn + h_up + [f_dn, f_up, h_own] + h_mate:
        cp.wait_send()
    o_mine.wait()
    o_mate.wait()


def attend(length, tokens, project, up, down):
    any_spec = pl.BlockSpec(memory_space=pl.ANY)
    dma = pltpu.SemaphoreType.DMA
    return pl.pallas_call(
        attend_kernel,
        name="attend",
        out_shape=(
            jax.ShapeDtypeStruct((512, 1024), BF),
            jax.ShapeDtypeStruct((2, 1024, 4096), BF),
        ),
        in_specs=[pl.BlockSpec(memory_space=pltpu.SMEM)] + [any_spec] * 4,
        out_specs=(any_spec, any_spec),
        scratch_shapes=[
            pltpu.VMEM((4, 1024, 1024), BF),
            pltpu.VMEM((1024, 1536), BF),
            pltpu.VMEM((4, KB, 256), BF),
            pltpu.VMEM((8, 80, KB), BF),
            pltpu.VMEM((8, 256, 1024), BF),
            pltpu.VMEM((8, 80, 1024), F32),
            pltpu.VMEM((8, 1, 1024), F32),
            pltpu.VMEM((KB, 1024), F32),
            pltpu.VMEM((2, 1, 1024), F32),
            pltpu.VMEM((1024, 512), BF),
            pltpu.VMEM((2, 64, 4096), BF),
            dma((8,)), dma((6,)), dma((6,)), dma((7,)), dma((7,)),
            dma((2, 20)), dma((2, 4, 4, 2)), dma((2, 4, 4)), dma((2, 4, 4)), dma((3,)),
        ],
        compiler_params=pltpu.CompilerParams(
            collective_id=0, has_side_effects=True, vmem_limit_bytes=62 * 2**20
        ),
    )(length, tokens, project, up, down)


def layer_norm(values, gain, shift):
    average = jnp.mean(values, axis=-1, keepdims=True)
    centred = values - average
    variance = jnp.mean(centred * centred, axis=-1, keepdims=True)
    return centred * lax.rsqrt(variance + 1e-05) * gain + shift


FC = 1024
RB = 512


def feed_kernel(
    len_ref, att_ref, tok_ref, wo_ref, g1_ref, b1_ref, g2_ref, b2_ref, up_ref, dn_ref, out_ref, tot_ref, normed, acc
):
    i = pl.program_id(0)

    @pl.when(i == 0)
    def _():
        for r in range(512 // RB):
            rows = pl.ds(r * RB, RB)
            mixed = jnp.dot(att_ref[rows, :], wo_ref[...], preferred_element_type=F32)
            mixed = mixed + tok_ref[rows, :].astype(F32)
            n = layer_norm(mixed, g1_ref[...], b1_ref[...]).astype(BF)
            normed[rows, :] = n
            acc[rows, :] = n.astype(F32)

    for r in range(512 // RB):
        rows = pl.ds(r * RB, RB)
        h = jnp.dot(normed[rows, :], up_ref[0], preferred_element_type=F32)
        inner = (0.5 * h * (1.0 + lax.erf(h * math.sqrt(0.5)))).astype(BF)
        acc[rows, :] += lax.dot_general(
            inner, dn_ref[0], (((1,), (1,)), ((), ())), preferred_element_type=F32
        )

    @pl.when(i == 4096 // FC - 1)
    def _():
        total = jnp.zeros((1, 1024), F32)
        for r in range(512 // RB):
            rows = pl.ds(r * RB, RB)
            final = layer_norm(acc[rows, :], g2_ref[...], b2_ref[...])
            out_ref[rows, :] = final.astype(BF)
            pos = lax.broadcasted_iota(jnp.int32, (RB, 1), 0) + (lax.axis_index("seq") * 512 + r * RB)
            valid = (pos < len_ref[0]).astype(F32)
            total = total + jnp.sum(final * valid, axis=0, keepdims=True)
        tot_ref[...] = total


def feed(lengths, att, tokens, output_weight, rows, wf):
    whole = lambda shape: pl.BlockSpec(shape, lambda i: (0,) * len(shape))
    return pl.pallas_call(
        feed_kernel,
        name="feed",
        grid=(4096 // FC,),
        out_shape=(jax.ShapeDtypeStruct((512, 1024), BF), jax.ShapeDtypeStruct((1, 1024), F32)),
        in_specs=[
            pl.BlockSpec(memory_space=pltpu.SMEM),
            whole((512, 1024)),
            whole((512, 1024)),
            whole((1024, 1024)),
            *[whole((1, 1024))] * 4,
            pl.BlockSpec((1, 1024, FC), lambda i: (0, 0, i)),
            pl.BlockSpec((1, 1024, FC), lambda i: (1, 0, i)),
        ],
        out_specs=(whole((512, 1024)), whole((1, 1024))),
        scratch_shapes=[pltpu.VMEM((512, 1024), BF), pltpu.VMEM((512, 1024), F32)],
        compiler_params=pltpu.CompilerParams(
            dimension_semantics=("arbitrary",), vmem_limit_bytes=56 * 2**20
        ),
    )(lengths, att, tokens, output_weight, *rows, wf, wf)


def loss_kernel(len_ref, pos_ref, tot_ref, q_ref, emb_ref, loss_ref, parts, sent, passages, ssem, rsem, ssem2, rsem2):
    s = lax.axis_index("seq")
    g = lax.axis_index("grp")
    barrier = pltpu.get_barrier_semaphore()
    for d in range(1, 8):
        pl.semaphore_signal(barrier, inc=1, device_id={"seq": lax.rem(s + d, 8)}, device_id_type=MESH)
    for d in range(1, 16):
        pl.semaphore_signal(barrier, inc=1, device_id={"grp": lax.rem(g + d, 16)}, device_id_type=MESH)
    pl.semaphore_wait(barrier, 22)
    first = []
    for d in range(1, 8):
        cp = pltpu.make_async_remote_copy(
            src_ref=tot_ref, dst_ref=parts.at[d], send_sem=ssem.at[d], recv_sem=rsem.at[d],
            device_id={"seq": lax.rem(s + d, 8)}, device_id_type=MESH,
        )
        cp.start()
        first.append(cp)
    qv = q_ref[...]
    short_q = (qv / jnp.sqrt(jnp.sum(qv * qv, axis=-1, keepdims=True) + 1e-06)).astype(BF)
    for cp in first:
        cp.wait_recv()
    total = tot_ref[...]
    for d in range(1, 8):
        total = total + parts[d]
    pooled = total / len_ref[0].astype(F32)
    emb = pooled / jnp.sqrt(jnp.sum(pooled * pooled, axis=-1, keepdims=True) + 1e-06)
    emb_ref[...] = emb
    sent[...] = emb
    second = []
    for d in range(1, 16):
        cp = pltpu.make_async_remote_copy(
            src_ref=sent, dst_ref=passages.at[d], send_sem=ssem2.at[d], recv_sem=rsem2.at[d],
            device_id={"grp": lax.rem(g + d, 16)}, device_id_type=MESH,
        )
        cp.start()
        second.append(cp)
    for cp in second:
        cp.wait_recv()
    rows = [emb] + [passages[d] for d in range(1, 16)]
    allp = jnp.concatenate(rows, axis=0).astype(BF)
    logits = 20.0 * lax.dot_general(
        allp, short_q, (((1,), (1,)), ((), ())), preferred_element_type=F32
    )
    ids = lax.rem(g + 16 - lax.broadcasted_iota(jnp.int32, (16, 8), 0), 16)
    picked = jnp.sum(jnp.where(pos_ref[...] == ids, logits, 0.0), axis=0, keepdims=True)
    loss_ref[...] = jnp.log(jnp.sum(jnp.exp(logits), axis=0, keepdims=True)) - picked
    for cp in first + second:
        cp.wait_send()


def losses(length, positive, total, queries):
    vm = pl.BlockSpec(memory_space=pltpu.VMEM)
    dma = pltpu.SemaphoreType.DMA
    return pl.pallas_call(
        loss_kernel,
        name="losses",
        out_shape=(jax.ShapeDtypeStruct((1, 1024), F32), jax.ShapeDtypeStruct((1, 8), F32)),
        in_specs=[pl.BlockSpec(memory_space=pltpu.SMEM), vm, vm, vm],
        out_specs=(vm, vm),
        scratch_shapes=[
            pltpu.VMEM((8, 1, 1024), F32),
            pltpu.VMEM((1, 1024), F32),
            pltpu.VMEM((16, 1, 1024), F32),
            dma((8,)), dma((8,)), dma((16,)), dma((16,)),
        ],
        compiler_params=pltpu.CompilerParams(collective_id=1, has_side_effects=True),
    )(length, positive, total, queries)


def body(
    hidden_in, lengths, project_weight, output_weight, first_gain, first_shift,
    up_weight, down_weight, second_gain, second_shift, queries, positive,
):
    tokens = hidden_in[0]
    att, wf = attend(lengths, tokens, project_weight, up_weight, down_weight)
    rows = [v[None, :] for v in (first_gain, first_shift, second_gain, second_shift)]
    final, total = feed(lengths, att, tokens, output_weight, rows, wf)
    embedding, loss = losses(lengths, positive[None, :], total, queries)
    return final[None], embedding, loss[0]


def solution(mesh):
    in_specs = (
        P("grp", "seq", None), P("grp"), P(), P(), P(), P(),
        P("grp", None), P("grp", None), P(), P(), P("grp", None), P("grp"),
    )
    out_specs = (P("grp", "seq", None), P("grp", None), P("grp"))
    return jax.shard_map(body, mesh=mesh, in_specs=in_specs, out_specs=out_specs, check_vma=False)
```

```python
import math
import functools

import jax
import jax.numpy as jnp
from jax import lax
from jax.experimental import pallas as pl
from jax.experimental.pallas import tpu as pltpu
from jax.sharding import PartitionSpec as P

MESH = pl.DeviceIdType.MESH
BF = jnp.bfloat16
F32 = jnp.float32
NEG = -1e30
KB = 1024
RS = 256
EV = (2, 2, 2, 2, 11, 11, 14, 18, 18, 25, 25, 30, 30, 30)
SCALE = math.log2(math.e) / 8.0


def attend_kernel(
    len_ref, x_ref, w_ref, up_ref, dn_ref, att_ref, wf_ref,
    xbuf, wqkv, kscr, vscr, qscr, acc, mx, sbuf, al, stage, wv,
    lsem, hs, hr, ds, dr, ws, wr, ps, pr, osem,
):
    s = lax.axis_index("seq")
    g = lax.axis_index("grp")
    c = lax.rem(s, 2)
    z = s // 2
    gx = lax.rem(g, 4)
    gy = g // 4
    mate = {"seq": s + 1 - 2 * c}
    zup = {"seq": lax.rem(s + 2, 8)}
    zdn = {"seq": lax.rem(s + 6, 8)}

    def wrap(v):
        return lax.rem(v, 4)

    def peer(axis, step):
        if axis == 0:
            return {"grp": gy * 4 + wrap(gx + step)}
        return {"grp": wrap(gy + step) * 4 + gx}

    loads = [pltpu.make_async_copy(x_ref, xbuf.at[0, pl.ds(0, 512)], lsem.at[0])]
    for t in range(3):
        cols = pl.ds(pl.multiple_of(t * 1024 + c * 512, 512), 512)
        loads.append(
            pltpu.make_async_copy(w_ref.at[:, cols], wqkv.at[:, pl.ds(t * 512, 512)], lsem.at[1 + t])
        )
    loads.append(pltpu.make_async_copy(up_ref, wv.at[0], lsem.at[4]))
    loads.append(pltpu.make_async_copy(dn_ref, wv.at[1], lsem.at[5]))
    for cp in loads:
        cp.start()

    peers = [mate, zup, zdn, peer(0, 1), peer(0, 3), peer(1, 1), peer(1, 3)]
    barrier = pltpu.get_barrier_semaphore()
    for d in peers:
        pl.semaphore_signal(barrier, inc=1, device_id=d, device_id_type=MESH)
    pl.semaphore_wait(barrier, len(peers))

    def rcopy(src, dst, ssem, rsem, dev):
        return pltpu.make_async_remote_copy(
            src_ref=src, dst_ref=dst, send_sem=ssem, recv_sem=rsem, device_id=dev, device_id_type=MESH
        )

    def h_piece(p):
        return xbuf.at[0, pl.ds(p * 256, 256)]

    def x_quarter(j, q):
        return xbuf.at[j, pl.ds(q * 256, 256)]

    h_own = rcopy(xbuf.at[0, pl.ds(0, 512)], xbuf.at[0, pl.ds(512, 512)], ds.at[0], dr.at[0], mate)
    h_dn = [rcopy(h_piece(p), x_quarter(1 + p, 0), hs.at[p], hr.at[p], zdn) for p in range(2)]
    h_up = [rcopy(h_piece(p), x_quarter(1 + p, 2), hs.at[2 + p], hr.at[2 + p], zup) for p in range(2)]
    f_dn = rcopy(x_quarter(1, 0), x_quarter(3, 0), hs.at[4], hr.at[4], zdn)
    f_up = rcopy(x_quarter(2, 2), x_quarter(3, 1), hs.at[5], hr.at[5], zup)
    h_mate = []
    for k, (j, a, b) in enumerate([(1, 0, 1), (1, 2, 3), (2, 0, 1), (2, 2, 3), (3, 0, 2), (3, 1, 3)]):
        h_mate.append(rcopy(x_quarter(j, a), x_quarter(j, b), ds.at[1 + k], dr.at[1 + k], mate))

    def origin_row(t, d1, d2):
        dx, dy = (d1, d2) if t == 0 else (d2, d1)
        return (wrap(gy + dy) * 4 + wrap(gx + dx)) * 64 + t * 32

    def w_reg(t, d1, d2, lo, n):
        return wf_ref.at[c, pl.ds(pl.multiple_of(origin_row(t, d1, d2) + lo, 16), n), :]

    w1, w2, w3, w4 = {}, {}, {}, {}
    for t in range(2):
        mine = wv.at[c, pl.ds(t * 32, 32), :]
        a1, a2 = t, 1 - t
        for i, (step, seen) in enumerate([(1, 3), (3, 1)]):
            w1[t, i] = rcopy(mine, w_reg(t, 0, 0, 0, 32), ws.at[t, i], wr.at[t, seen, 0, 0], peer(a1, step))
            w2[t, i] = rcopy(
                w_reg(t, seen, 0, 16 * i, 16), w_reg(t, seen, 0, 16 * i, 16),
                ws.at[t, 2 + i], wr.at[t, 2, 0, i], peer(a1, step),
            )
            for d1 in range(4):
                src = mine if d1 == 0 else w_reg(t, d1, 0, 0, 32)
                w3[t, d1, i] = rcopy(
                    src, w_reg(t, d1, 0, 0, 32), ws.at[t, 4 + 2 * d1 + i], wr.at[t, d1, seen, 0], peer(a2, step)
                )
                w4[t, d1, i] = rcopy(
                    w_reg(t, d1, seen, 16 * i, 16), w_reg(t, d1, seen, 16 * i, 16),
                    ws.at[t, 12 + 2 * d1 + i], wr.at[t, d1, 2, i], peer(a2, step),
                )
    w5 = {}
    for t in range(2):
        for d1 in range(4):
            for d2 in range(4):
                if d1 or d2:
                    w5[t, d1, d2] = rcopy(
                        w_reg(t, d1, d2, 0, 32), w_reg(t, d1, d2, 0, 32),
                        ps.at[t, d1, d2], pr.at[t, d1, d2], mate,
                    )

    def w_arrived(t, d1, d2, k, n):
        reg = w_reg(t, d1, d2, 16 * k, n)
        pltpu.make_async_copy(reg, reg, wr.at[t, d1, d2, k]).wait()

    loads[0].wait()
    for cp in h_dn + h_up + [h_own]:
        cp.start()
    loads[4].wait()
    loads[5].wait()
    for t in range(2):
        for i in range(2):
            w1[t, i].start()
    for t in range(2):
        for i in range(2):
            w3[t, 0, i].start()
    own_rows = pl.ds(pl.multiple_of(g * 64, 64), 64)
    outs = [pltpu.make_async_copy(wv.at[k], wf_ref.at[k, own_rows, :], lsem.at[6 + k]) for k in range(2)]
    for cp in outs:
        cp.start()

    qscr[...] = jnp.zeros_like(qscr)
    for h in range(8):
        qscr[h, 128:144, :] = (lax.broadcasted_iota(jnp.int32, (16, KB), 0) == 0).astype(BF)
        vscr[h, 64:80, :] = jnp.ones((16, KB), BF)
    acc[...] = jnp.zeros_like(acc)
    mx[...] = jnp.full_like(mx, NEG)
    length = len_ref[0]

    for k in range(3):
        loads[1 + k].wait()
    h_own.wait_recv()
    for i in range(2):
        q = jnp.dot(xbuf[0], wqkv[:, 256 * i : 256 * i + 256], preferred_element_type=F32)
        qt = (q * SCALE).T.astype(BF)
        for u in range(4):
            h = 4 * i + u
            qscr[h, (u % 2) * 64 : (u % 2) * 64 + 64, :] = qt[64 * u : 64 * u + 64]

    def score_rows(h, r):
        rows = pl.ds(r * RS, RS)
        sc = jnp.dot(kscr[h // 2, rows, :], qscr[h], preferred_element_type=F32)
        sbuf[rows, :] = sc
        return jnp.max(sc.reshape(RS // 8, 8, 1024), axis=0)

    def new_max(h, tops):
        top = functools.reduce(jnp.maximum, tops)
        old = mx[h]
        new = jnp.maximum(old, jnp.max(top, axis=0, keepdims=True))
        mx[h] = new
        al[0] = jnp.exp2(old - new)
        al[1] = new

    def head_step(h, following):
        factor = al[0]
        top = al[1]
        tops = []
        out = None
        for r in range(KB // RS):
            p = jnp.exp2(sbuf[pl.ds(r * RS, RS), :] - top).astype(BF)
            if following is not None:
                tops.append(score_rows(following, r))
            part = jnp.dot(vscr[h, :, pl.ds(r * RS, RS)], p, preferred_element_type=F32)
            out = part if out is None else out + part
        if following is not None:
            new_max(following, tops)
        acc[h] = acc[h] * factor + out

    def events(e):
        def at(k, fn):
            @pl.when(e == k)
            def _():
                fn()

        def hidden_next(j):
            if j == 1:
                h_dn[0].wait_recv()
                h_up[0].wait_recv()
                f_dn.start()
                h_mate[0].start()
                h_mate[1].start()
            elif j == 2:
                h_dn[1].wait_recv()
                h_up[1].wait_recv()
                f_up.start()
                h_mate[2].start()
                h_mate[3].start()
            else:
                f_dn.wait_recv()
                f_up.wait_recv()
                h_mate[4].start()
                h_mate[5].start()

        def arrived(*blocks):
            for t in range(2):
                for d1, d2 in blocks:
                    if d1 == 2 and d2 == 0 or d2 == 2:
                        w_arrived(t, d1, d2, 0, 16)
                        w_arrived(t, d1, d2, 1, 16)
                    else:
                        w_arrived(t, d1, d2, 0, 32)

        def send(group, *d1s):
            for t in range(2):
                for i in range(2):
                    if d1s:
                        for d1 in d1s:
                            group[t, d1, i].start()
                    else:
                        group[t, i].start()

        def share(*blocks):
            for t in range(2):
                for d1, d2 in blocks:
                    w5[t, d1, d2].start()

        def e1():
            arrived((1, 0), (3, 0))
            send(w2)

        def e3():
            share((1, 0), (3, 0))

        def e5():
            arrived((0, 1), (0, 3))
            send(w4, 0)
            share((0, 1), (0, 3))

        def e6():
            arrived((2, 0))
            send(w3, 2)
            share((2, 0))

        def e8():
            arrived((1, 1), (1, 3))
            send(w4, 1)
            share((1, 1), (1, 3))

        def e9():
            arrived((3, 1), (3, 3))
            send(w4, 3)
            share((3, 1), (3, 3))

        def e10():
            arrived((0, 2))
            share((0, 2))

        def e11():
            arrived((2, 1), (2, 3))
            send(w4, 2)
            share((2, 1), (2, 3))

        def last(d1):
            arrived((d1, 2))
            share((d1, 2))

        at(EV[0], e1)
        at(EV[1], lambda: send(w3, 1))
        at(EV[2], e3)
        at(EV[3], lambda: send(w3, 3))
        at(EV[4], e5)
        at(EV[5], e6)
        at(12, lambda: hidden_next(2))
        at(5, lambda: hidden_next(1))
        at(20, lambda: hidden_next(3))
        at(EV[7], e8)
        at(EV[8], e9)
        at(EV[9], e10)
        at(EV[10], e11)
        at(EV[11], lambda: last(1))
        at(EV[12], lambda: last(3))
        at(EV[13], lambda: last(2))

    def chunk(j, carry):
        for k in range(1, 4):

            @pl.when(j == k)
            def _():
                h_mate[2 * k - 2].wait_recv()
                h_mate[2 * k - 1].wait_recv()

        edge = jnp.logical_or(j == 0, j == 3).astype(jnp.int32)
        for q in range(4):
            dz = edge * jnp.where(j == 0, 0, 2) + (1 - edge) * (1 if q < 2 else 3)
            cc = edge * (q // 2) + (1 - edge) * (q % 2)
            pp = edge * (q % 2) + (1 - edge) * (j - 1)
            base = (wrap(z + dz) * 2 + c + cc - 2 * c * cc) * 512 + pp * 256
            pos = lax.broadcasted_iota(jnp.int32, (256, 128), 0) + base
            bias = jnp.where(pos < length, 0.0, NEG).astype(BF)
            for pr_ in range(4):
                kscr[pr_, q * 256 : q * 256 + 256, 128:256] = bias
        xj = xbuf[j]
        for i in range(2):
            kk = jnp.dot(xj, wqkv[:, 512 + 256 * i : 768 + 256 * i], preferred_element_type=F32).astype(BF)
            kscr[2 * i, :, 0:128] = kk[:, 0:128]
            kscr[2 * i + 1, :, 0:128] = kk[:, 128:256]
            vt = jnp.dot(xj, wqkv[:, 1024 + 256 * i : 1280 + 256 * i], preferred_element_type=F32).T.astype(BF)
            for u in range(4):
                vscr[4 * i + u, 0:64, :] = vt[64 * u : 64 * u + 64]

        new_max(0, [score_rows(0, r) for r in range(KB // RS)])

        def it(h, carry2):
            events(j * 8 + h)
            head_step(h, h + 1)
            return carry2

        lax.fori_loop(0, 7, it, 0)
        head_step(7, None)
        return carry

    lax.fori_loop(0, 4, chunk, 0)

    for pr_ in range(4):
        pair = []
        for h in (2 * pr_, 2 * pr_ + 1):
            pair.append(acc[h, 0:64, :] / acc[h, 64:65, :])
        both = jnp.concatenate(pair, axis=0)
        stage[:, 128 * pr_ : 128 * pr_ + 128] = both.T.astype(BF)
    my_cols = pl.ds(pl.multiple_of(c * 512, 512), 512)
    o_mate = rcopy(stage.at[pl.ds(512, 512)], att_ref.at[:, my_cols], osem.at[0], osem.at[1], mate)
    o_mine = pltpu.make_async_copy(stage.at[pl.ds(0, 512)], att_ref.at[:, my_cols], osem.at[2])
    o_mate.start()
    o_mine.start()
    for cp in w5.values():
        cp.wait()
    for group in (w1, w2, w3, w4):
        for cp in group.values():
            cp.wait_send()
    for cp in outs:
        cp.wait()
    for cp in h_dn + h_up + [f_dn, f_up, h_own] + h_mate:
        cp.wait_send()
    o_mine.wait()
    o_mate.wait()


def attend(length, tokens, project, up, down):
    any_spec = pl.BlockSpec(memory_space=pl.ANY)
    dma = pltpu.SemaphoreType.DMA
    return pl.pallas_call(
        attend_kernel,
        name="attend",
        out_shape=(
            jax.ShapeDtypeStruct((512, 1024), BF),
            jax.ShapeDtypeStruct((2, 1024, 4096), BF),
        ),
        in_specs=[pl.BlockSpec(memory_space=pltpu.SMEM)] + [any_spec] * 4,
        out_specs=(any_spec, any_spec),
        scratch_shapes=[
            pltpu.VMEM((4, 1024, 1024), BF),
            pltpu.VMEM((1024, 1536), BF),
            pltpu.VMEM((4, KB, 256), BF),
            pltpu.VMEM((8, 80, KB), BF),
            pltpu.VMEM((8, 256, 1024), BF),
            pltpu.VMEM((8, 80, 1024), F32),
            pltpu.VMEM((8, 1, 1024), F32),
            pltpu.VMEM((KB, 1024), F32),
            pltpu.VMEM((2, 1, 1024), F32),
            pltpu.VMEM((1024, 512), BF),
            pltpu.VMEM((2, 64, 4096), BF),
            dma((8,)), dma((6,)), dma((6,)), dma((7,)), dma((7,)),
            dma((2, 20)), dma((2, 4, 4, 2)), dma((2, 4, 4)), dma((2, 4, 4)), dma((3,)),
        ],
        compiler_params=pltpu.CompilerParams(
            collective_id=0, has_side_effects=True, vmem_limit_bytes=62 * 2**20
        ),
    )(length, tokens, project, up, down)


def layer_norm(values, gain, shift):
    average = jnp.mean(values, axis=-1, keepdims=True)
    centred = values - average
    variance = jnp.mean(centred * centred, axis=-1, keepdims=True)
    return centred * lax.rsqrt(variance + 1e-05) * gain + shift


FC = 1024
RB = 512


def feed_kernel(
    len_ref, att_ref, tok_ref, wo_ref, g1_ref, b1_ref, g2_ref, b2_ref, up_ref, dn_ref, out_ref, tot_ref, normed, acc
):
    i = pl.program_id(0)

    @pl.when(i == 0)
    def _():
        for r in range(512 // RB):
            rows = pl.ds(r * RB, RB)
            mixed = jnp.dot(att_ref[rows, :], wo_ref[...], preferred_element_type=F32)
            mixed = mixed + tok_ref[rows, :].astype(F32)
            n = layer_norm(mixed, g1_ref[...], b1_ref[...]).astype(BF)
            normed[rows, :] = n
            acc[rows, :] = n.astype(F32)

    for r in range(512 // RB):
        rows = pl.ds(r * RB, RB)
        h = jnp.dot(normed[rows, :], up_ref[0], preferred_element_type=F32)
        inner = (0.5 * h * (1.0 + lax.erf(h * math.sqrt(0.5)))).astype(BF)
        acc[rows, :] += lax.dot_general(
            inner, dn_ref[0], (((1,), (1,)), ((), ())), preferred_element_type=F32
        )

    @pl.when(i == 4096 // FC - 1)
    def _():
        total = jnp.zeros((1, 1024), F32)
        for r in range(512 // RB):
            rows = pl.ds(r * RB, RB)
            final = layer_norm(acc[rows, :], g2_ref[...], b2_ref[...])
            out_ref[rows, :] = final.astype(BF)
            pos = lax.broadcasted_iota(jnp.int32, (RB, 1), 0) + (lax.axis_index("seq") * 512 + r * RB)
            valid = (pos < len_ref[0]).astype(F32)
            total = total + jnp.sum(final * valid, axis=0, keepdims=True)
        tot_ref[...] = total


def feed(lengths, att, tokens, output_weight, rows, wf):
    whole = lambda shape: pl.BlockSpec(shape, lambda i: (0,) * len(shape))
    return pl.pallas_call(
        feed_kernel,
        name="feed",
        grid=(4096 // FC,),
        out_shape=(jax.ShapeDtypeStruct((512, 1024), BF), jax.ShapeDtypeStruct((1, 1024), F32)),
        in_specs=[
            pl.BlockSpec(memory_space=pltpu.SMEM),
            whole((512, 1024)),
            whole((512, 1024)),
            whole((1024, 1024)),
            *[whole((1, 1024))] * 4,
            pl.BlockSpec((1, 1024, FC), lambda i: (0, 0, i)),
            pl.BlockSpec((1, 1024, FC), lambda i: (1, 0, i)),
        ],
        out_specs=(whole((512, 1024)), whole((1, 1024))),
        scratch_shapes=[pltpu.VMEM((512, 1024), BF), pltpu.VMEM((512, 1024), F32)],
        compiler_params=pltpu.CompilerParams(
            dimension_semantics=("arbitrary",), vmem_limit_bytes=56 * 2**20
        ),
    )(lengths, att, tokens, output_weight, *rows, wf, wf)


def loss_kernel(len_ref, pos_ref, tot_ref, q_ref, emb_ref, loss_ref, parts, sent, passages, ssem, rsem, ssem2, rsem2):
    s = lax.axis_index("seq")
    g = lax.axis_index("grp")
    barrier = pltpu.get_barrier_semaphore()
    for d in range(1, 8):
        pl.semaphore_signal(barrier, inc=1, device_id={"seq": lax.rem(s + d, 8)}, device_id_type=MESH)
    for d in range(1, 16):
        pl.semaphore_signal(barrier, inc=1, device_id={"grp": lax.rem(g + d, 16)}, device_id_type=MESH)
    pl.semaphore_wait(barrier, 22)
    first = []
    for d in range(1, 8):
        cp = pltpu.make_async_remote_copy(
            src_ref=tot_ref, dst_ref=parts.at[d], send_sem=ssem.at[d], recv_sem=rsem.at[d],
            device_id={"seq": lax.rem(s + d, 8)}, device_id_type=MESH,
        )
        cp.start()
        first.append(cp)
    qv = q_ref[...]
    short_q = (qv / jnp.sqrt(jnp.sum(qv * qv, axis=-1, keepdims=True) + 1e-06)).astype(BF)
    for cp in first:
        cp.wait_recv()
    total = tot_ref[...]
    for d in range(1, 8):
        total = total + parts[d]
    pooled = total / len_ref[0].astype(F32)
    emb = pooled / jnp.sqrt(jnp.sum(pooled * pooled, axis=-1, keepdims=True) + 1e-06)
    emb_ref[...] = emb
    sent[...] = emb
    second = []
    for d in range(1, 16):
        cp = pltpu.make_async_remote_copy(
            src_ref=sent, dst_ref=passages.at[d], send_sem=ssem2.at[d], recv_sem=rsem2.at[d],
            device_id={"grp": lax.rem(g + d, 16)}, device_id_type=MESH,
        )
        cp.start()
        second.append(cp)
    for cp in second:
        cp.wait_recv()
    rows = [emb] + [passages[d] for d in range(1, 16)]
    allp = jnp.concatenate(rows, axis=0).astype(BF)
    logits = 20.0 * lax.dot_general(
        allp, short_q, (((1,), (1,)), ((), ())), preferred_element_type=F32
    )
    ids = lax.rem(g + 16 - lax.broadcasted_iota(jnp.int32, (16, 8), 0), 16)
    picked = jnp.sum(jnp.where(pos_ref[...] == ids, logits, 0.0), axis=0, keepdims=True)
    loss_ref[...] = jnp.log(jnp.sum(jnp.exp(logits), axis=0, keepdims=True)) - picked
    for cp in first + second:
        cp.wait_send()


def losses(length, positive, total, queries):
    vm = pl.BlockSpec(memory_space=pltpu.VMEM)
    dma = pltpu.SemaphoreType.DMA
    return pl.pallas_call(
        loss_kernel,
        name="losses",
        out_shape=(jax.ShapeDtypeStruct((1, 1024), F32), jax.ShapeDtypeStruct((1, 8), F32)),
        in_specs=[pl.BlockSpec(memory_space=pltpu.SMEM), vm, vm, vm],
        out_specs=(vm, vm),
        scratch_shapes=[
            pltpu.VMEM((8, 1, 1024), F32),
            pltpu.VMEM((1, 1024), F32),
            pltpu.VMEM((16, 1, 1024), F32),
            dma((8,)), dma((8,)), dma((16,)), dma((16,)),
        ],
        compiler_params=pltpu.CompilerParams(collective_id=1, has_side_effects=True),
    )(length, positive, total, queries)


def body(
    hidden_in, lengths, project_weight, output_weight, first_gain, first_shift,
    up_weight, down_weight, second_gain, second_shift, queries, positive,
):
    tokens = hidden_in[0]
    att, wf = attend(lengths, tokens, project_weight, up_weight, down_weight)
    rows = [v[None, :] for v in (first_gain, first_shift, second_gain, second_shift)]
    final, total = feed(lengths, att, tokens, output_weight, rows, wf)
    embedding, loss = losses(lengths, positive[None, :], total, queries)
    return final[None], embedding, loss[0]


def solution(mesh):
    in_specs = (
        P("grp", "seq", None), P("grp"), P(), P(), P(), P(),
        P("grp", None), P("grp", None), P(), P(), P("grp", None), P("grp"),
    )
    out_specs = (P("grp", "seq", None), P("grp", None), P("grp"))
    return jax.shard_map(body, mesh=mesh, in_specs=in_specs, out_specs=out_specs, check_vma=False)
```
